256 devices in a mesh: frames: 64 (over z, x, core), mp: 4 (over y).
Axes of the slice: x: 4, y: 4, z: 8, core: 2. Of those that a mesh axis runs over, the one named last changes fastest.
Arguments:
- features: bfloat16 [8192, 512], P('frames'), may hold values from -32 to 32
- logit_weight: bfloat16 [512, 640], replicated, may hold values from -1 to 1
- gumbel_perturbation: float32 [8192, 640], P('frames'), may hold values from -3 to 12
- codebook: bfloat16 [640, 384], replicated, may hold values from -6 to 6
- project_weight: bfloat16 [768, 768], P(None, 'mp'), may hold values from -0.21875 to 0.21875
- context: bfloat16 [8192, 768], P('frames', 'mp'), may hold values from -6 to 6
- distractors: int32 [8192, 100], P('frames'), may hold values from 0 to 8191, as said below
- masked: int32 [8192], P('frames'), may hold values from 0 to 1
Outputs:
- scores: float32 [8192, 101], P('frames')
- loss: float32 [], replicated
- diversity: float32 [], replicated
The draws below stay inside these ranges and needn't reach their ends.
Inputs may be any that keep to these rules, and one draw needn't show every extreme that they name: `distractors`: the distractor of a frame in shard s (frames s * 128 to s * 128 + 127) lies in shard s + o modulo 8192 // 128, with 1 <= |o| <= 3.
All inputs are finite; a program needn't handle non-finite values.
Results may differ from the reference program's by a relative error of at most 0.0049.
Values may be sent and summed in bfloat16 or wider, within the bound.
No kernel may reach another device: no remote copies, remote signals or barrier semaphores. Data moves between devices by JAX's collectives and lax.ppermute only.
A program may use at most 64 MiB of HBM per device.

```python
import math
import jax
import jax.numpy as jnp
from jax import lax

FEAT = 512
V = 320
DQ = 768
G = 2
NEG = 100
REACH = 3
TOK_DEV = 128
TOKENS = 8192


def shared_weight(key):
    return jax.random.normal(jax.random.fold_in(key, 11), (FEAT, G * V), jnp.float32) / math.sqrt(FEAT)


def draw_logit_weight(key, part):
    return jnp.clip(shared_weight(key), -1.0, 1.0).astype(jnp.bfloat16)


def draw_features(key, part):
    noise = jax.random.normal(jax.random.fold_in(key, 12), (TOKENS, FEAT), jnp.float32)
    drift = jax.random.normal(jax.random.fold_in(key, 13), (FEAT,), jnp.float32)
    ramp = (2.0 * (jnp.arange(TOKENS, dtype=jnp.float32) + 0.5) / TOKENS - 1.0)[:, None]
    base = noise + 2.0 * ramp * drift[None, :]
    return jnp.clip(base, -32.0, 32.0).astype(jnp.bfloat16)


def draw_gumbel_perturbation(key, part):
    return jnp.clip(jax.random.gumbel(jax.random.fold_in(key, 21), (TOKENS, G * V), jnp.float32), -3.0, 12.0)


def draw_distractors(key, part):
    shards = TOKENS // TOK_DEV
    shard = jnp.arange(TOKENS, dtype=jnp.int32) // TOK_DEV
    choose = jax.random.randint(jax.random.fold_in(key, 31), (TOKENS, NEG), 0, 2 * REACH)
    offset = jnp.where(choose < REACH, choose + 1, REACH - 1 - choose)
    source = (shard[:, None] + offset + shards) % shards
    within = jax.random.randint(jax.random.fold_in(key, 32), (TOKENS, NEG), 0, TOK_DEV)
    return (source * TOK_DEV + within).astype(jnp.int32)


def draw_masked(key, part):
    draw_value = jax.random.randint(jax.random.fold_in(key, 41), (TOKENS,), 0, 1000)
    level = 250 + 500 * jnp.arange(TOKENS, dtype=jnp.int32) // TOKENS
    return (draw_value < level).astype(jnp.int32)


def shard_levels(rng, dims, split, smallest, high):
    factor_of = 1.0
    for dim, shards_of in split:
        heights = jax.random.uniform(jax.random.fold_in(jax.random.fold_in(rng, 6), dim), (shards_of,), jnp.float32, smallest / len(split), high / len(split))
        factor_of = factor_of * jnp.repeat(jnp.exp(heights), dims[dim] // shards_of).reshape((-1,) + (1,) * (len(dims) - 1 - dim))
    return factor_of


def centred(own_key, dims, scale, reach, cuts=(), kind=jnp.bfloat16):
    values = jax.random.normal(own_key, dims, jnp.float32) * scale
    if len(cuts) > 0:
        values = shard_levels(own_key, dims, cuts, -0.22, 0.18) * values
    return jnp.clip(values, min=-reach, max=reach).astype(kind)


def setup_inputs(seed: int = 0) -> dict:
    key_list = jax.random.split(jax.random.key(seed), 9)
    return {
        "features": draw_features(jax.random.fold_in(key_list[8], 71), 0),
        "logit_weight": draw_logit_weight(jax.random.fold_in(key_list[8], 71), 0),
        "gumbel_perturbation": draw_gumbel_perturbation(jax.random.fold_in(key_list[8], 71), 0),
        "codebook": centred(key_list[3], (G * V, DQ // G), 1.0, 6.0),
        "project_weight": centred(key_list[4], (DQ, DQ), DQ ** -0.5, 0.21875, ((1, 4),)),
        "context": centred(key_list[5], (TOKENS, DQ), 1.0, 6.0, ((0, 64), (1, 4))),
        "distractors": draw_distractors(jax.random.fold_in(key_list[8], 71), 0),
        "masked": draw_masked(jax.random.fold_in(key_list[8], 71), 0),
    }


gumbel_softness = 2.0
logit_softness = 0.1
norm_epsilon = 1e-06

def grouped_softmax(values):
    count = values.shape[0]
    shaped = values.reshape(count, G, -1)
    top = lax.optimization_barrier(jnp.max(shaped, axis=2, keepdims=True))
    expd = jnp.exp(shaped - top)
    return (expd / lax.optimization_barrier(jnp.sum(expd, axis=2, keepdims=True))).reshape(count, -1)

def reference(features, logit_weight, gumbel_perturbation, codebook, project_weight, context, distractors, masked):
    codeword_logits = jnp.dot(features.astype(jnp.float32), logit_weight.astype(jnp.float32), preferred_element_type=jnp.float32)
    clean = grouped_softmax(codeword_logits)
    usage = lax.optimization_barrier(jnp.mean(clean, axis=0)).reshape(G, V)
    perplex = jnp.sum(jnp.exp(-lax.optimization_barrier(jnp.sum(usage * jnp.log(usage + 1e-07), axis=1))))
    diversity = (G * V - perplex) / (G * V)
    soft_assignment = grouped_softmax((codeword_logits + gumbel_perturbation) / gumbel_softness).astype(jnp.bfloat16)
    pieces = [jnp.dot(soft_assignment[:, g * V:(g + 1) * V].astype(jnp.float32), codebook[g * V:(g + 1) * V].astype(jnp.float32), preferred_element_type=jnp.float32) for g in range(G)]
    codevec = jnp.concatenate(pieces, axis=1).astype(jnp.bfloat16)
    target = jnp.dot(codevec.astype(jnp.float32), project_weight.astype(jnp.float32), preferred_element_type=jnp.float32)
    unit = (target * lax.rsqrt(lax.optimization_barrier(jnp.sum(target * target, axis=1)) + norm_epsilon)[:, None]).astype(jnp.bfloat16)
    ctx_float = context.astype(jnp.float32)
    context_squared = lax.optimization_barrier(jnp.sum(ctx_float * ctx_float, axis=1))
    self_dot = lax.optimization_barrier(jnp.sum(ctx_float * unit.astype(jnp.float32), axis=1))
    block = math.gcd(context.shape[0], 128)
    ctx_blocks = context.reshape(-1, block, DQ)
    idx_blocks = distractors.reshape(-1, block, NEG)

    def one_block(pair):
        ctx_part, idx_part = pair
        taken = unit[idx_part.astype(jnp.int32)].astype(jnp.float32)
        return jnp.einsum('td,tkd->tk', ctx_part.astype(jnp.float32), taken)
    other_dot = lax.map(one_block, (ctx_blocks, idx_blocks)).reshape(-1, NEG)
    inner_products = jnp.concatenate([self_dot[:, None], other_dot], axis=1)
    scores = inner_products * lax.rsqrt(context_squared + norm_epsilon)[:, None] / logit_softness
    cross = jnp.log(lax.optimization_barrier(jnp.sum(jnp.exp(scores), axis=1))) - scores[:, 0]
    loss = jnp.sum(jnp.where(masked == 1, cross, jnp.float32(0.0))) / scores.shape[0]
    return (scores, loss, diversity)
```

```python
import functools

import jax
import jax.numpy as jnp
from jax import lax
from jax.experimental import pallas as pl
from jax.experimental.pallas import tpu as pltpu
from jax.sharding import PartitionSpec as P


V = 320
G = 2
NEG = 100
GUMBEL_SOFTNESS = 2.0
LOGIT_SOFTNESS = 0.1
NORM_EPSILON = 1e-06

F32 = jnp.float32
BF16 = jnp.bfloat16
I32 = jnp.int32

BLOCK_OFFSETS = (1, -2, -1, -3, 3, 2)
BLOCKS = len(BLOCK_OFFSETS)

SELF_ROW = 100
CTX_ROW = 101
OWN_NORM_ROW = 102
NORM_ROW = 104
PAYLOAD_ROWS = 112

VMEM = pltpu.MemorySpace.VMEM
SMEM = pltpu.MemorySpace.SMEM
HBM = pltpu.MemorySpace.HBM
PARAMS = pltpu.CompilerParams(vmem_limit_bytes=8 << 20)


def group_shift(values, first):
    low = jnp.max(jnp.where(first, values, -jnp.inf), axis=1, keepdims=True)
    high = jnp.max(jnp.where(first, -jnp.inf, values), axis=1, keepdims=True)
    return jnp.where(first, low, high)


def group_softmax(values, first):
    powers = jnp.exp(values - group_shift(values, first))
    low = jnp.sum(jnp.where(first, powers, 0.0), axis=1, keepdims=True)
    high = jnp.sum(jnp.where(first, 0.0, powers), axis=1, keepdims=True)
    return powers * jnp.where(first, 1.0 / low, 1.0 / high)


def target_kernel(
    feat_hbm, lw_hbm, gum_hbm, cb_hbm, wt_hbm, ctxt_hbm, mask_hbm, idxt_hbm,
    tgt_ref, rows_ref, probs_ref, ctx_ref, code_kt_ref, code_tk_ref,
    feat, lw, gum, cb, wt, ctxt, mask, idxt, sems,
):
    copies = [
        pltpu.make_async_copy(src, dst, sems.at[i])
        for i, (src, dst) in enumerate((
            (feat_hbm, feat), (lw_hbm, lw), (gum_hbm, gum), (cb_hbm, cb),
            (wt_hbm, wt), (ctxt_hbm, ctxt), (mask_hbm, mask),
            (idxt_hbm, idxt.at[pl.ds(0, NEG)]),
        ))
    ]
    for copy in copies:
        copy.start()
    own = lax.axis_index("frames")
    sign = 1 - 2 * lax.rem(own, 2)
    copies[0].wait()
    copies[1].wait()
    logits = jnp.dot(feat[...], lw[...], preferred_element_type=F32)
    lane = lax.broadcasted_iota(I32, logits.shape, 1)
    first = lane < V
    copies[2].wait()
    soft = group_softmax((logits + gum[...]) / GUMBEL_SOFTNESS, first)
    soft_low = jnp.where(first, soft, 0.0).astype(BF16)
    soft_high = jnp.where(first, 0.0, soft).astype(BF16)
    copies[3].wait()
    codevec = jnp.concatenate(
        [
            jnp.dot(soft_low[:, :384], cb[0:384, :], preferred_element_type=F32).astype(BF16),
            jnp.dot(soft_high[:, 256:], cb[256:640, :], preferred_element_type=F32).astype(BF16),
        ],
        axis=1,
    )
    copies[4].wait()
    target = lax.dot_general(
        wt[...], codevec, (((1,), (1,)), ((), ())), preferred_element_type=F32
    )
    target = target.astype(BF16)
    tgt_ref[...] = target
    probs_ref[...] = jnp.sum(group_softmax(logits, first), axis=0, keepdims=True)
    copies[5].wait()
    wide = target.astype(F32)
    context = ctxt[...].astype(F32)
    rows_ref[...] = jnp.zeros_like(rows_ref)
    rows_ref[0:1, :] = jnp.sum(wide * context, axis=0, keepdims=True)
    rows_ref[1:2, :] = jnp.sum(context * context, axis=0, keepdims=True)
    rows_ref[2:3, :] = jnp.sum(wide * wide, axis=0, keepdims=True)
    ctx_ref[...] = jnp.transpose(context).astype(BF16)
    copies[6].wait()
    rows_ref[3:4, :] = mask[...].astype(F32)
    copies[7].wait()
    row = lax.broadcasted_iota(I32, idxt.shape, 0)
    index = jnp.where(row < NEG, idxt[...], 0)
    offset = ((((index >> 7) - own + 32) & 63) - 32) * sign
    block = jnp.zeros_like(index)
    for i, o in enumerate(BLOCK_OFFSETS):
        block = jnp.where(offset == o, i, block)
    code = (index & 127) + (block << 7)
    code_kt_ref[...] = code
    code_tk_ref[...] = jnp.transpose(code)


def lane_pick(values, index):
    return jnp.take_along_axis(values, index, axis=1, mode="promise_in_bounds")


def dots_kernel(w_ref, a_ref, b_ref, c_ref, d_ref, e_ref, ctx_ref, code_ref, rows_ref, out_ref):
    ctx = ctx_ref[...]
    code = code_ref[...]
    local = code & 127
    block = code >> 7
    out_ref[SELF_ROW : SELF_ROW + 4, :] = rows_ref[0:4, :]
    out_ref[NORM_ROW:, :] = jnp.zeros((PAYLOAD_ROWS - NORM_ROW, 128), F32)
    picked = jnp.zeros(code.shape, F32)
    for i, ref in enumerate((w_ref, a_ref, b_ref, c_ref, d_ref, e_ref)):
        target = ref[...]
        sims = jnp.dot(ctx, target, preferred_element_type=F32)
        picked = jnp.where(block == i, lane_pick(sims, local), picked)
        wide = target.astype(F32)
        out_ref[NORM_ROW + i : NORM_ROW + i + 1, :] = jnp.sum(wide * wide, axis=0, keepdims=True)
    out_ref[0:NEG, :] = jnp.transpose(picked)[0:NEG, :]


def scores_kernel(p0, p1, p2, p3, code_ref, rows_ref, probs_ref, scores_ref, parts_ref):
    total = (p0[...] + p1[...]) + (p2[...] + p3[...])
    scale = lax.rsqrt(total[CTX_ROW : CTX_ROW + 1, :] + NORM_EPSILON) / LOGIT_SOFTNESS
    inverse = lax.rsqrt(total[OWN_NORM_ROW:, :] + NORM_EPSILON)
    own = total[SELF_ROW : SELF_ROW + 1, :] * inverse[0:1, :] * scale
    code = code_ref[0:104, :]
    local = code & 127
    block = code >> 7
    picked = jnp.zeros(code.shape, F32)
    for i in range(BLOCKS):
        at = NORM_ROW - OWN_NORM_ROW + i
        table = jnp.broadcast_to(inverse[at : at + 1, :], code.shape)
        picked = jnp.where(block == i, lane_pick(table, local), picked)
    others = total[0:104, :] * picked * scale
    row = lax.broadcasted_iota(I32, others.shape, 0)
    powers = jnp.where(row < NEG, jnp.exp(jnp.where(row < NEG, others, 0.0)), 0.0)
    summed = jnp.sum(powers, axis=0, keepdims=True) + jnp.exp(own)
    cross = jnp.where(rows_ref[3:4, :] == 1.0, jnp.log(summed) - own, 0.0)
    scores_ref[0:1, :] = own
    scores_ref[1 : NEG + 1, :] = others[0:NEG, :]
    line = jnp.concatenate([probs_ref[...], cross], axis=1)
    parts_ref[...] = jnp.broadcast_to(line[None], parts_ref.shape)


def totals_kernel(frames, parts_ref, loss_ref, diversity_ref):
    total = jnp.sum(parts_ref[...], axis=0) / frames
    usage = total[:, : G * V]
    lane = lax.broadcasted_iota(I32, usage.shape, 1)
    terms = usage * jnp.log(usage + 1e-07)
    low = jnp.sum(jnp.where(lane < V, terms, 0.0), axis=1, keepdims=True)
    high = jnp.sum(jnp.where(lane < V, 0.0, terms), axis=1, keepdims=True)
    perplex = jnp.exp(-low) + jnp.exp(-high)
    diversity_ref[...] = (G * V - perplex) / (G * V)
    loss_ref[...] = jnp.sum(total[:, G * V :], axis=1, keepdims=True)


def struct(shape, kind):
    return jax.ShapeDtypeStruct(shape, kind)


def exchange(value, shards, replicas, source):
    pairs = []
    for s in range(shards):
        for j in range(replicas):
            pairs.append((source(s) % shards * replicas + j, s * replicas + j))
    return lax.ppermute(value, ("frames", "mp"), pairs)


def on_device(
    features, logit_weight, gumbel, codebook, project_weight, context, distractors, masked
):
    count = features.shape[0]
    shards = lax.axis_size("frames")
    replicas = lax.axis_size("mp")
    weight_t = project_weight.T
    context_t = context.T
    width = context_t.shape[0]
    operands = (
        features, logit_weight, gumbel, codebook, weight_t, context_t, masked.reshape(1, count)
    )
    target, rows, probs, ctx, code_kt, code_tk = pl.pallas_call(
        target_kernel,
        out_shape=(
            struct((width, count), BF16),
            struct((8, count), F32),
            struct((1, G * V), F32),
            struct((count, width), BF16),
            struct((128, count), I32),
            struct((count, 128), I32),
        ),
        in_specs=[pl.BlockSpec(memory_space=HBM)] * 8,
        out_specs=[pl.BlockSpec(memory_space=VMEM)] * 6,
        scratch_shapes=[pltpu.VMEM(x.shape, x.dtype) for x in operands]
        + [pltpu.VMEM((128, count), I32), pltpu.SemaphoreType.DMA((8,))],
        compiler_params=PARAMS,
        name="target",
    )(*[pltpu.with_memory_space_constraint(x, HBM) for x in (*operands, distractors.T)])

    def side(s):
        return -1 if s % 2 == 0 else 1

    send = functools.partial(exchange, shards=shards, replicas=replicas)
    b = send(target, source=lambda s: (s + 2 * side(s)) ^ 1)
    c = send(target, source=lambda s: (s + 4 * side(s)) ^ 1)
    a = send(target, source=lambda s: s + 2 * side(s))
    w = send(target, source=lambda s: s ^ 1)
    a, b, c = lax.optimization_barrier((a, b, c))
    d = send(a, source=lambda s: s ^ 1)
    e = send(b, source=lambda s: s ^ 1)
    payload = pl.pallas_call(
        dots_kernel,
        out_shape=struct((PAYLOAD_ROWS, count), F32),
        in_specs=[pl.BlockSpec(memory_space=VMEM)] * 9,
        out_specs=pl.BlockSpec(memory_space=VMEM),
        compiler_params=PARAMS,
        name="dots",
    )(w, a, b, c, d, e, ctx, code_tk, rows)
    peers = [
        lax.ppermute(payload, "mp", [((j + step) % replicas, j) for j in range(replicas)])
        for step in range(1, replicas)
    ]
    scores_t, parts = pl.pallas_call(
        scores_kernel,
        out_shape=(struct((NEG + 1, count), F32), struct((shards, 1, G * V + count), F32)),
        in_specs=[pl.BlockSpec(memory_space=VMEM)] * 7,
        out_specs=[pl.BlockSpec(memory_space=VMEM)] * 2,
        compiler_params=PARAMS,
        name="scores",
    )(payload, *peers, code_kt, rows, probs)
    parts = lax.all_to_all(parts, "frames", split_axis=0, concat_axis=0, tiled=True)
    loss, diversity = pl.pallas_call(
        functools.partial(totals_kernel, count * shards),
        out_shape=(struct((1, 1), F32), struct((1, 1), F32)),
        in_specs=[pl.BlockSpec(memory_space=VMEM)],
        out_specs=[pl.BlockSpec(memory_space=VMEM)] * 2,
        compiler_params=PARAMS,
        name="totals",
    )(parts)
    return scores_t.T, loss.reshape(()), diversity.reshape(())


def solution(mesh):
    return jax.shard_map(
        on_device,
        mesh=mesh,
        in_specs=(
            P("frames", None),
            P(),
            P("frames", None),
            P(),
            P(None, "mp"),
            P("frames", "mp"),
            P("frames", None),
            P("frames"),
        ),
        out_specs=(P("frames", None), P(), P()),
        check_vma=False,
    )
```

```python
import functools

import jax
import jax.numpy as jnp
from jax import lax
from jax.experimental import pallas as pl
from jax.experimental.pallas import tpu as pltpu
from jax.sharding import PartitionSpec as P


V = 320
G = 2
NEG = 100
GUMBEL_SOFTNESS = 2.0
LOGIT_SOFTNESS = 0.1
NORM_EPSILON = 1e-06

F32 = jnp.float32
BF16 = jnp.bfloat16
I32 = jnp.int32

BLOCK_OFFSETS = (1, -2, -1, -3, 3, 2)
BLOCKS = len(BLOCK_OFFSETS)

SELF_ROW = 100
CTX_ROW = 101
OWN_NORM_ROW = 102
NORM_ROW = 104
PAYLOAD_ROWS = 112

PROB_ROWS = 16
CLASSES = 8
CUT = 16
LOSS_LANE = 80

VMEM = pltpu.MemorySpace.VMEM
SMEM = pltpu.MemorySpace.SMEM
HBM = pltpu.MemorySpace.HBM
PARAMS = pltpu.CompilerParams(vmem_limit_bytes=8 << 20)


def group_stats(values, first, reduce, empty):
    head = values[:, : V - V % 128]
    middle = values[:, V - V % 128 : V - V % 128 + 128]
    tail = values[:, V - V % 128 + 128 :]
    low = reduce(
        jnp.concatenate([head, jnp.where(first, middle, empty)], axis=1), axis=1, keepdims=True
    )
    high = reduce(
        jnp.concatenate([jnp.where(first, empty, middle), tail], axis=1), axis=1, keepdims=True
    )
    return low, high


def by_group(low, high, first):
    count = first.shape[0]
    return jnp.concatenate(
        [
            jnp.broadcast_to(low, (count, V - V % 128)),
            jnp.where(first, low, high),
            jnp.broadcast_to(high, (count, V - V % 128)),
        ],
        axis=1,
    )


def group_softmax(values, first):
    shift = by_group(*group_stats(values, first, jnp.max, -jnp.inf), first)
    powers = jnp.exp(values - shift)
    low, high = group_stats(powers, first, jnp.sum, 0.0)
    return powers * by_group(1.0 / low, 1.0 / high, first)


def bf16_parts(values):
    high = values.astype(BF16).astype(F32)
    middle = (values - high).astype(BF16).astype(F32)
    return high, middle, values - high - middle


def target_kernel(
    feat_hbm, lw_hbm, gum_hbm, cb_hbm, wt_hbm, ctxt_hbm, mask_hbm, idxt_hbm,
    tgt_ref, rows_ref, ctx_ref, code_kt_ref, code_tk_ref,
    feat, lw, gum, cb, wt, ctxt, mask, idxt, sems,
):
    copies = [
        pltpu.make_async_copy(src, dst, sems.at[i])
        for i, (src, dst) in enumerate((
            (feat_hbm, feat), (lw_hbm, lw), (gum_hbm, gum), (cb_hbm, cb),
            (wt_hbm, wt), (ctxt_hbm, ctxt), (mask_hbm, mask),
            (idxt_hbm, idxt.at[pl.ds(0, NEG)]),
        ))
    ]
    for copy in copies:
        copy.start()
    own = lax.axis_index("frames")
    sign = 1 - 2 * lax.rem(own, 2)
    copies[0].wait()
    copies[1].wait()
    logits = jnp.dot(feat[...], lw[...], preferred_element_type=F32)
    first = lax.broadcasted_iota(I32, (logits.shape[0], 128), 1) < V % 128
    copies[2].wait()
    soft = group_softmax((logits + gum[...]) / GUMBEL_SOFTNESS, first)
    middle = soft[:, 256:384]
    soft_low = jnp.concatenate([soft[:, :256], jnp.where(first, middle, 0.0)], axis=1)
    soft_high = jnp.concatenate([jnp.where(first, 0.0, middle), soft[:, 384:]], axis=1)
    copies[3].wait()
    codevec = jnp.concatenate(
        [
            jnp.dot(part.astype(BF16), cb[at : at + 384, :], preferred_element_type=F32)
            for part, at in ((soft_low, 0), (soft_high, 256))
        ],
        axis=1,
    ).astype(BF16)
    copies[4].wait()
    target = lax.dot_general(
        wt[...], codevec, (((1,), (1,)), ((), ())), preferred_element_type=F32
    )
    target = target.astype(BF16)
    width = target.shape[0]
    tgt_ref[0:width, :] = target
    probs = jnp.sum(group_softmax(logits, first), axis=0, keepdims=True)
    tgt_ref[width:, :] = jnp.concatenate(
        [
            part[:, at : at + 128]
            for part in bf16_parts(probs)
            for at in range(0, G * V, 128)
        ]
        + [jnp.zeros((1, 128), F32)],
        axis=0,
    ).astype(BF16)
    copies[5].wait()
    wide = target.astype(F32)
    context = ctxt[...].astype(F32)
    rows_ref[...] = jnp.zeros_like(rows_ref)
    rows_ref[0:1, :] = jnp.sum(wide * context, axis=0, keepdims=True)
    rows_ref[1:2, :] = jnp.sum(context * context, axis=0, keepdims=True)
    rows_ref[2:3, :] = jnp.sum(wide * wide, axis=0, keepdims=True)
    ctx_ref[...] = jnp.transpose(context).astype(BF16)
    copies[6].wait()
    rows_ref[3:4, :] = mask[...].astype(F32)
    copies[7].wait()
    row = lax.broadcasted_iota(I32, idxt.shape, 0)
    index = jnp.where(row < NEG, idxt[...], 0)
    offset = ((((index >> 7) - own + 32) & 63) - 32) * sign
    block = jnp.zeros_like(index)
    for i, o in enumerate(BLOCK_OFFSETS):
        block = jnp.where(offset == o, i, block)
    code = (index & 127) + (block << 7)
    code_kt_ref[...] = code
    code_tk_ref[...] = jnp.transpose(code)


def lane_pick(values, index):
    return jnp.take_along_axis(values, index, axis=1, mode="promise_in_bounds")


def dots_kernel(
    own_ref, w_ref, a_ref, b_ref, c_ref, d_ref, e_ref, ctx_ref, code_ref, rows_ref,
    out_ref, probs_ref,
):
    ctx = ctx_ref[...]
    width = ctx.shape[1]
    code = code_ref[...]
    local = code & 127
    block = code >> 7
    out_ref[SELF_ROW : SELF_ROW + 4, :] = rows_ref[0:4, :]
    out_ref[NORM_ROW:, :] = jnp.zeros((PAYLOAD_ROWS - NORM_ROW, 128), F32)
    picked = jnp.zeros(code.shape, F32)
    probs = own_ref[width:, :].astype(F32) + d_ref[width + PROB_ROWS :, :].astype(F32)
    for i, ref in enumerate((w_ref, a_ref, b_ref, c_ref, d_ref, e_ref)):
        target = ref[0:width, :]
        sims = jnp.dot(ctx, target, preferred_element_type=F32)
        picked = jnp.where(block == i, lane_pick(sims, local), picked)
        wide = target.astype(F32)
        out_ref[NORM_ROW + i : NORM_ROW + i + 1, :] = jnp.sum(wide * wide, axis=0, keepdims=True)
        probs = probs + ref[width : width + PROB_ROWS, :].astype(F32)
    out_ref[0:NEG, :] = jnp.transpose(picked)[0:NEG, :]
    probs_ref[...] = jnp.zeros_like(probs_ref)
    probs_ref[0:5, :] = probs[0:5, :] + (probs[5:10, :] + probs[10:15, :])


def scores_kernel(p0, p1, p2, p3, code_ref, rows_ref, probs_ref, scores_ref, parts_ref):
    total = (p0[...] + p1[...]) + (p2[...] + p3[...])
    scale = lax.rsqrt(total[CTX_ROW : CTX_ROW + 1, :] + NORM_EPSILON) / LOGIT_SOFTNESS
    inverse = lax.rsqrt(total[OWN_NORM_ROW:, :] + NORM_EPSILON)
    own = total[SELF_ROW : SELF_ROW + 1, :] * inverse[0:1, :] * scale
    code = code_ref[0:104, :]
    local = code & 127
    block = code >> 7
    picked = jnp.zeros(code.shape, F32)
    for i in range(BLOCKS):
        at = NORM_ROW - OWN_NORM_ROW + i
        table = jnp.broadcast_to(inverse[at : at + 1, :], code.shape)
        picked = jnp.where(block == i, lane_pick(table, local), picked)
    others = total[0:104, :] * picked * scale
    row = lax.broadcasted_iota(I32, others.shape, 0)
    powers = jnp.where(row < NEG, jnp.exp(jnp.where(row < NEG, others, 0.0)), 0.0)
    summed = jnp.sum(powers, axis=0, keepdims=True) + jnp.exp(own)
    cross = jnp.where(rows_ref[3:4, :] == 1.0, jnp.log(summed) - own, 0.0)
    scores_ref[0:1, :] = own
    scores_ref[1 : NEG + 1, :] = others[0:NEG, :]
    cut = lax.rem(lax.axis_index("frames"), CLASSES)
    rolled = pltpu.roll(probs_ref[...], 128 - CUT * cut, 1)
    row = lax.broadcasted_iota(I32, rolled.shape, 0)
    lane = lax.broadcasted_iota(I32, rolled.shape, 1)
    line = jnp.where((lane >> 4) + row == 0, rolled, 0.0)
    for i in range(1, G * V // 128):
        here = ((lane >> 4) == i) & (row == i)
        line = jnp.where(here, pltpu.roll(rolled, CUT * i, 1), line)
    line = jnp.sum(line, axis=0, keepdims=True)
    lane = lax.broadcasted_iota(I32, line.shape, 1)
    line = jnp.where(
        lane < LOSS_LANE, line,
        jnp.where(lane == LOSS_LANE, jnp.sum(cross, axis=1, keepdims=True), 0.0),
    )
    parts_ref[...] = jnp.broadcast_to(line[None], parts_ref.shape)


def totals_kernel(frames, parts_ref, loss_ref, diversity_ref):
    parts = parts_ref[...]
    parts = parts.reshape(parts.shape[0] // CLASSES, CLASSES, 1, 128)
    total = jnp.sum(parts, axis=0) / frames
    cut = lax.broadcasted_iota(I32, total.shape, 0)
    lane = lax.broadcasted_iota(I32, total.shape, 2)
    column = (lane >> 4) * 128 + cut * CUT + (lane & 15)
    counted = lane < LOSS_LANE
    usage = jnp.where(counted, total, 0.0)
    terms = usage * jnp.log(usage + 1e-07)

    def summed(where):
        rows = jnp.sum(jnp.where(where, terms, 0.0), axis=0)
        return jnp.sum(rows, axis=1, keepdims=True)

    perplex = jnp.exp(-summed(column < V)) + jnp.exp(-summed(column >= V))
    diversity_ref[...] = (G * V - perplex) / (G * V)
    loss = jnp.sum(jnp.where(lane == LOSS_LANE, total, 0.0), axis=0)
    loss_ref[...] = jnp.sum(loss, axis=1, keepdims=True)


def struct(shape, kind):
    return jax.ShapeDtypeStruct(shape, kind)


def exchange(value, shards, replicas, source):
    pairs = []
    for s in range(shards):
        for j in range(replicas):
            pairs.append((source(s) % shards * replicas + j, s * replicas + j))
    return lax.ppermute(value, ("frames", "mp"), pairs)


def on_device(
    features, logit_weight, gumbel, codebook, project_weight, context, distractors, masked
):
    count = features.shape[0]
    shards = lax.axis_size("frames")
    replicas = lax.axis_size("mp")
    weight_t = project_weight.T
    context_t = context.T
    width = context_t.shape[0]
    operands = (
        features, logit_weight, gumbel, codebook, weight_t, context_t, masked.reshape(1, count)
    )
    target, rows, ctx, code_kt, code_tk = pl.pallas_call(
        target_kernel,
        out_shape=(
            struct((width + PROB_ROWS, count), BF16),
            struct((8, count), F32),
            struct((count, width), BF16),
            struct((128, count), I32),
            struct((count, 128), I32),
        ),
        in_specs=[pl.BlockSpec(memory_space=HBM)] * 8,
        out_specs=[pl.BlockSpec(memory_space=VMEM)] * 5,
        scratch_shapes=[pltpu.VMEM(x.shape, x.dtype) for x in operands]
        + [pltpu.VMEM((128, count), I32), pltpu.SemaphoreType.DMA((8,))],
        compiler_params=PARAMS,
        name="target",
    )(*[pltpu.with_memory_space_constraint(x, HBM) for x in (*operands, distractors.T)])

    def side(s):
        return -1 if s % 2 == 0 else 1

    send = functools.partial(exchange, shards=shards, replicas=replicas)
    b = send(target, source=lambda s: (s + 2 * side(s)) ^ 1)
    c = send(target, source=lambda s: (s + 4 * side(s)) ^ 1)
    a = send(target, source=lambda s: s + 2 * side(s))
    w = send(target, source=lambda s: s ^ 1)
    a, b, c, w = lax.optimization_barrier((a, b, c, w))
    d = send(jnp.concatenate([a, c[width:]], axis=0), source=lambda s: s ^ 1)
    e = send(b, source=lambda s: s ^ 1)
    payload, probs = pl.pallas_call(
        dots_kernel,
        out_shape=(struct((PAYLOAD_ROWS, count), F32), struct((8, 128), F32)),
        in_specs=[pl.BlockSpec(memory_space=VMEM)] * 10,
        out_specs=[pl.BlockSpec(memory_space=VMEM)] * 2,
        compiler_params=PARAMS,
        name="dots",
    )(target, w, a, b, c, d, e, ctx, code_tk, rows)
    peers = [
        lax.ppermute(payload, "mp", [(j ^ step, j) for j in range(replicas)])
        for step in range(replicas - 1, 0, -1)
    ]
    scores_t, parts = pl.pallas_call(
        scores_kernel,
        out_shape=(struct((NEG + 1, count), F32), struct((shards, 1, 128), F32)),
        in_specs=[pl.BlockSpec(memory_space=VMEM)] * 7,
        out_specs=[pl.BlockSpec(memory_space=VMEM)] * 2,
        compiler_params=PARAMS,
        name="scores",
    )(payload, *reversed(peers), code_kt, rows, probs)
    parts = lax.all_to_all(parts, "frames", split_axis=0, concat_axis=0, tiled=True)
    loss, diversity = pl.pallas_call(
        functools.partial(totals_kernel, count * shards),
        out_shape=(struct((1, 1), F32), struct((1, 1), F32)),
        in_specs=[pl.BlockSpec(memory_space=VMEM)],
        out_specs=[pl.BlockSpec(memory_space=VMEM)] * 2,
        compiler_params=PARAMS,
        name="totals",
    )(parts)
    return scores_t.T, loss.reshape(()), diversity.reshape(())


def solution(mesh):
    return jax.shard_map(
        on_device,
        mesh=mesh,
        in_specs=(
            P("frames", None),
            P(),
            P("frames", None),
            P(),
            P(None, "mp"),
            P("frames", "mp"),
            P("frames", None),
            P("frames"),
        ),
        out_specs=(P("frames", None), P(), P()),
        check_vma=False,
    )
```

```python
import functools

import jax
import jax.numpy as jnp
from jax import lax
from jax.experimental import pallas as pl
from jax.experimental.pallas import tpu as pltpu
from jax.sharding import PartitionSpec as P


V = 320
G = 2
NEG = 100
GUMBEL_SOFTNESS = 2.0
LOGIT_SOFTNESS = 0.1
NORM_EPSILON = 1e-06

F32 = jnp.float32
BF16 = jnp.bfloat16
I32 = jnp.int32

BLOCKS = 6

SELF_ROW = 100
CTX_ROW = 101
OWN_NORM_ROW = 102
NORM_ROW = 104
PAYLOAD_ROWS = 112

PROB_ROWS = 16
CLASSES = 8
CUT = 16
LOSS_LANE = 80

VMEM = pltpu.MemorySpace.VMEM
SMEM = pltpu.MemorySpace.SMEM
HBM = pltpu.MemorySpace.HBM
PARAMS = pltpu.CompilerParams(vmem_limit_bytes=8 << 20)


def group_stats(values, first, reduce, empty):
    head = values[:, : V - V % 128]
    middle = values[:, V - V % 128 : V - V % 128 + 128]
    tail = values[:, V - V % 128 + 128 :]
    low = reduce(
        jnp.concatenate([head, jnp.where(first, middle, empty)], axis=1), axis=1, keepdims=True
    )
    high = reduce(
        jnp.concatenate([jnp.where(first, empty, middle), tail], axis=1), axis=1, keepdims=True
    )
    return low, high


def by_group(low, high, first):
    count = first.shape[0]
    return jnp.concatenate(
        [
            jnp.broadcast_to(low, (count, V - V % 128)),
            jnp.where(first, low, high),
            jnp.broadcast_to(high, (count, V - V % 128)),
        ],
        axis=1,
    )


def group_softmax(values, first):
    shift = by_group(*group_stats(values, first, jnp.max, -jnp.inf), first)
    powers = jnp.exp(values - shift)
    low, high = group_stats(powers, first, jnp.sum, 0.0)
    return powers * by_group(1.0 / low, 1.0 / high, first)


def bf16_parts(values):
    high = values.astype(BF16).astype(F32)
    middle = (values - high).astype(BF16).astype(F32)
    return high, middle, values - high - middle


def target_kernel(
    feat_hbm, lw_hbm, gum_hbm, cb_hbm, wt_hbm, ctxt_hbm, mask_hbm, idxt_hbm,
    tgt_ref, rows_ref, ctx_ref, code_kt_ref, code_tk_ref,
    feat, lw, gum, cb, wt, ctxt, mask, idxt, sems,
):
    copies = [
        pltpu.make_async_copy(src, dst, sems.at[i])
        for i, (src, dst) in enumerate((
            (feat_hbm, feat), (lw_hbm, lw), (gum_hbm, gum), (cb_hbm, cb),
            (wt_hbm, wt), (ctxt_hbm, ctxt), (mask_hbm, mask),
            (idxt_hbm, idxt.at[pl.ds(0, NEG)]),
        ))
    ]
    for copy in copies:
        copy.start()
    own = lax.axis_index("frames")
    partner = 1 - 2 * lax.rem(own, 2)
    inner = 2 - 4 * lax.rem(own // 2, 2)
    distances = (partner, inner, -inner, -3 * partner, inner + partner, partner - inner)
    copies[0].wait()
    copies[1].wait()
    logits = jnp.dot(feat[...], lw[...], preferred_element_type=F32)
    first = lax.broadcasted_iota(I32, (logits.shape[0], 128), 1) < V % 128
    copies[2].wait()
    soft = group_softmax((logits + gum[...]) / GUMBEL_SOFTNESS, first)
    middle = soft[:, 256:384]
    soft_low = jnp.concatenate([soft[:, :256], jnp.where(first, middle, 0.0)], axis=1)
    soft_high = jnp.concatenate([jnp.where(first, 0.0, middle), soft[:, 384:]], axis=1)
    copies[3].wait()
    codevec = jnp.concatenate(
        [
            jnp.dot(part.astype(BF16), cb[at : at + 384, :], preferred_element_type=F32)
            for part, at in ((soft_low, 0), (soft_high, 256))
        ],
        axis=1,
    ).astype(BF16)
    copies[4].wait()
    target = lax.dot_general(
        wt[...], codevec, (((1,), (1,)), ((), ())), preferred_element_type=F32
    )
    target = target.astype(BF16)
    width = target.shape[0]
    tgt_ref[0:width, :] = target
    probs = jnp.sum(group_softmax(logits, first), axis=0, keepdims=True)
    tgt_ref[width:, :] = jnp.concatenate(
        [
            part[:, at : at + 128]
            for part in bf16_parts(probs)
            for at in range(0, G * V, 128)
        ]
        + [jnp.zeros((1, 128), F32)],
        axis=0,
    ).astype(BF16)
    copies[5].wait()
    wide = target.astype(F32)
    context = ctxt[...].astype(F32)
    rows_ref[...] = jnp.zeros_like(rows_ref)
    rows_ref[0:1, :] = jnp.sum(wide * context, axis=0, keepdims=True)
    rows_ref[1:2, :] = jnp.sum(context * context, axis=0, keepdims=True)
    rows_ref[2:3, :] = jnp.sum(wide * wide, axis=0, keepdims=True)
    ctx_ref[...] = jnp.transpose(context).astype(BF16)
    copies[6].wait()
    rows_ref[3:4, :] = mask[...].astype(F32)
    copies[7].wait()
    row = lax.broadcasted_iota(I32, idxt.shape, 0)
    index = jnp.where(row < NEG, idxt[...], 0)
    offset = (((index >> 7) - own + 32) & 63) - 32
    block = jnp.zeros_like(index)
    for i, o in enumerate(distances):
        block = jnp.where(offset == o, i, block)
    code = (index & 127) + (block << 7)
    code_kt_ref[...] = code
    code_tk_ref[...] = jnp.transpose(code)


def lane_pick(values, index):
    return jnp.take_along_axis(values, index, axis=1, mode="promise_in_bounds")


def dots_kernel(
    own_ref, w_ref, a_ref, b_ref, c_ref, d_ref, e_ref, ctx_ref, code_ref, rows_ref,
    out_ref, probs_ref,
):
    ctx = ctx_ref[...]
    width = ctx.shape[1]
    code = code_ref[...]
    local = code & 127
    block = code >> 7
    out_ref[SELF_ROW : SELF_ROW + 4, :] = rows_ref[0:4, :]
    out_ref[NORM_ROW:, :] = jnp.zeros((PAYLOAD_ROWS - NORM_ROW, 128), F32)
    picked = jnp.zeros(code.shape, F32)
    probs = own_ref[width:, :].astype(F32) + d_ref[width + PROB_ROWS :, :].astype(F32)
    for i, ref in enumerate((w_ref, a_ref, b_ref, c_ref, d_ref, e_ref)):
        target = ref[0:width, :]
        sims = jnp.dot(ctx, target, preferred_element_type=F32)
        picked = jnp.where(block == i, lane_pick(sims, local), picked)
        wide = target.astype(F32)
        out_ref[NORM_ROW + i : NORM_ROW + i + 1, :] = jnp.sum(wide * wide, axis=0, keepdims=True)
        probs = probs + ref[width : width + PROB_ROWS, :].astype(F32)
    out_ref[0:NEG, :] = jnp.transpose(picked)[0:NEG, :]
    probs_ref[...] = jnp.zeros_like(probs_ref)
    probs_ref[0:5, :] = probs[0:5, :] + (probs[5:10, :] + probs[10:15, :])


def scores_kernel(p0, p1, p2, p3, code_ref, rows_ref, probs_ref, scores_ref, parts_ref):
    total = (p0[...] + p1[...]) + (p2[...] + p3[...])
    scale = lax.rsqrt(total[CTX_ROW : CTX_ROW + 1, :] + NORM_EPSILON) / LOGIT_SOFTNESS
    inverse = lax.rsqrt(total[OWN_NORM_ROW:, :] + NORM_EPSILON)
    own = total[SELF_ROW : SELF_ROW + 1, :] * inverse[0:1, :] * scale
    code = code_ref[0:104, :]
    local = code & 127
    block = code >> 7
    picked = jnp.zeros(code.shape, F32)
    for i in range(BLOCKS):
        at = NORM_ROW - OWN_NORM_ROW + i
        table = jnp.broadcast_to(inverse[at : at + 1, :], code.shape)
        picked = jnp.where(block == i, lane_pick(table, local), picked)
    others = total[0:104, :] * picked * scale
    row = lax.broadcasted_iota(I32, others.shape, 0)
    powers = jnp.where(row < NEG, jnp.exp(jnp.where(row < NEG, others, 0.0)), 0.0)
    summed = jnp.sum(powers, axis=0, keepdims=True) + jnp.exp(own)
    cross = jnp.where(rows_ref[3:4, :] == 1.0, jnp.log(summed) - own, 0.0)
    scores_ref[0:1, :] = own
    scores_ref[1 : NEG + 1, :] = others[0:NEG, :]
    cut = lax.rem(lax.axis_index("frames"), CLASSES)
    rolled = pltpu.roll(probs_ref[...], 128 - CUT * cut, 1)
    row = lax.broadcasted_iota(I32, rolled.shape, 0)
    lane = lax.broadcasted_iota(I32, rolled.shape, 1)
    line = jnp.where((lane >> 4) + row == 0, rolled, 0.0)
    for i in range(1, G * V // 128):
        here = ((lane >> 4) == i) & (row == i)
        line = jnp.where(here, pltpu.roll(rolled, CUT * i, 1), line)
    line = jnp.sum(line, axis=0, keepdims=True)
    lane = lax.broadcasted_iota(I32, line.shape, 1)
    line = jnp.where(
        lane < LOSS_LANE, line,
        jnp.where(lane == LOSS_LANE, jnp.sum(cross, axis=1, keepdims=True), 0.0),
    )
    parts_ref[...] = jnp.broadcast_to(line[None], parts_ref.shape)


def totals_kernel(frames, parts_ref, loss_ref, diversity_ref):
    parts = parts_ref[...]
    parts = parts.reshape(parts.shape[0] // CLASSES, CLASSES, 1, 128)
    total = jnp.sum(parts, axis=0) / frames
    cut = lax.broadcasted_iota(I32, total.shape, 0)
    lane = lax.broadcasted_iota(I32, total.shape, 2)
    column = (lane >> 4) * 128 + cut * CUT + (lane & 15)
    counted = lane < LOSS_LANE
    usage = jnp.where(counted, total, 0.0)
    terms = usage * jnp.log(usage + 1e-07)

    def summed(where):
        rows = jnp.sum(jnp.where(where, terms, 0.0), axis=0)
        return jnp.sum(rows, axis=1, keepdims=True)

    perplex = jnp.exp(-summed(column < V)) + jnp.exp(-summed(column >= V))
    diversity_ref[...] = (G * V - perplex) / (G * V)
    loss = jnp.sum(jnp.where(lane == LOSS_LANE, total, 0.0), axis=0)
    loss_ref[...] = jnp.sum(loss, axis=1, keepdims=True)


def struct(shape, kind):
    return jax.ShapeDtypeStruct(shape, kind)


def exchange(value, shards, replicas, source):
    pairs = []
    for s in range(shards):
        for j in range(replicas):
            pairs.append((source(s) % shards * replicas + j, s * replicas + j))
    return lax.ppermute(value, ("frames", "mp"), pairs)


def on_device(
    features, logit_weight, gumbel, codebook, project_weight, context, distractors, masked
):
    count = features.shape[0]
    shards = lax.axis_size("frames")
    replicas = lax.axis_size("mp")
    weight_t = project_weight.T
    context_t = context.T
    width = context_t.shape[0]
    operands = (
        features, logit_weight, gumbel, codebook, weight_t, context_t, masked.reshape(1, count)
    )
    target, rows, ctx, code_kt, code_tk = pl.pallas_call(
        target_kernel,
        out_shape=(
            struct((width + PROB_ROWS, count), BF16),
            struct((8, count), F32),
            struct((count, width), BF16),
            struct((128, count), I32),
            struct((count, 128), I32),
        ),
        in_specs=[pl.BlockSpec(memory_space=HBM)] * 8,
        out_specs=[pl.BlockSpec(memory_space=VMEM)] * 5,
        scratch_shapes=[pltpu.VMEM(x.shape, x.dtype) for x in operands]
        + [pltpu.VMEM((128, count), I32), pltpu.SemaphoreType.DMA((8,))],
        compiler_params=PARAMS,
        name="target",
    )(*[pltpu.with_memory_space_constraint(x, HBM) for x in (*operands, distractors.T)])

    def outer(s):
        return s - 2 if s // 2 % 2 == 0 else s + 2

    def across(s):
        return s - 3 if s % 2 == 0 else s + 3

    send = functools.partial(exchange, shards=shards, replicas=replicas)
    b = send(target, source=outer)
    c = send(target, source=across)
    a = send(target, source=lambda s: s ^ 2)
    w = send(target, source=lambda s: s ^ 1)
    b, c, a, w = lax.optimization_barrier((b, c, a, w))
    d = send(jnp.concatenate([a, c[width:]], axis=0), source=lambda s: s ^ 1)
    e = send(b, source=lambda s: s ^ 1)
    payload, probs = pl.pallas_call(
        dots_kernel,
        out_shape=(struct((PAYLOAD_ROWS, count), F32), struct((8, 128), F32)),
        in_specs=[pl.BlockSpec(memory_space=VMEM)] * 10,
        out_specs=[pl.BlockSpec(memory_space=VMEM)] * 2,
        compiler_params=PARAMS,
        name="dots",
    )(target, w, a, b, c, d, e, ctx, code_tk, rows)
    peers = [
        lax.ppermute(payload, "mp", [(j ^ step, j) for j in range(replicas)])
        for step in (1, 3, 2)
    ]
    scores_t, parts = pl.pallas_call(
        scores_kernel,
        out_shape=(struct((NEG + 1, count), F32), struct((shards, 1, 128), F32)),
        in_specs=[pl.BlockSpec(memory_space=VMEM)] * 7,
        out_specs=[pl.BlockSpec(memory_space=VMEM)] * 2,
        compiler_params=PARAMS,
        name="scores",
    )(payload, *reversed(peers), code_kt, rows, probs)
    parts = lax.all_to_all(parts, "frames", split_axis=0, concat_axis=0, tiled=True)
    loss, diversity = pl.pallas_call(
        functools.partial(totals_kernel, count * shards),
        out_shape=(struct((1, 1), F32), struct((1, 1), F32)),
        in_specs=[pl.BlockSpec(memory_space=VMEM)],
        out_specs=[pl.BlockSpec(memory_space=VMEM)] * 2,
        compiler_params=PARAMS,
        name="totals",
    )(parts)
    return scores_t.T, loss.reshape(()), diversity.reshape(())


def solution(mesh):
    return jax.shard_map(
        on_device,
        mesh=mesh,
        in_specs=(
            P("frames", None),
            P(),
            P("frames", None),
            P(),
            P(None, "mp"),
            P("frames", "mp"),
            P("frames", None),
            P("frames"),
        ),
        out_specs=(P("frames", None), P(), P()),
        check_vma=False,
    )
```

```python
import functools

import jax
import jax.numpy as jnp
from jax import lax
from jax.experimental import pallas as pl
from jax.experimental.pallas import tpu as pltpu
from jax.sharding import PartitionSpec as P


V = 320
G = 2
NEG = 100
GUMBEL_SOFTNESS = 2.0
LOGIT_SOFTNESS = 0.1
NORM_EPSILON = 1e-06

F32 = jnp.float32
BF16 = jnp.bfloat16
I32 = jnp.int32

BLOCKS = 6

SELF_ROW = 100
CTX_ROW = 101
OWN_NORM_ROW = 102
NORM_ROW = 104
PAYLOAD_ROWS = 112

PROB_ROWS = 16
CLASSES = 8
CUT = 16
LOSS_LANE = 80

VMEM = pltpu.MemorySpace.VMEM
HBM = pltpu.MemorySpace.HBM
PARAMS = pltpu.CompilerParams(vmem_limit_bytes=8 << 20)


def group_stats(values, first, reduce, empty):
    head = values[:, : V - V % 128]
    middle = values[:, V - V % 128 : V - V % 128 + 128]
    tail = values[:, V - V % 128 + 128 :]
    low = reduce(
        jnp.concatenate([head, jnp.where(first, middle, empty)], axis=1), axis=1, keepdims=True
    )
    high = reduce(
        jnp.concatenate([jnp.where(first, empty, middle), tail], axis=1), axis=1, keepdims=True
    )
    return low, high


def by_group(low, high, first):
    count = first.shape[0]
    return jnp.concatenate(
        [
            jnp.broadcast_to(low, (count, V - V % 128)),
            jnp.where(first, low, high),
            jnp.broadcast_to(high, (count, V - V % 128)),
        ],
        axis=1,
    )


def group_softmax(values, first):
    shift = by_group(*group_stats(values, first, jnp.max, -jnp.inf), first)
    powers = jnp.exp(values - shift)
    low, high = group_stats(powers, first, jnp.sum, 0.0)
    return powers * by_group(1.0 / low, 1.0 / high, first)


def bf16_parts(values):
    high = values.astype(BF16).astype(F32)
    middle = (values - high).astype(BF16).astype(F32)
    return high, middle, values - high - middle


def target_kernel(feat_hbm, lw_hbm, gum_hbm, cb_hbm, wt_hbm, tgt_ref, feat, lw, gum, cb, wt, sems):
    copies = [
        pltpu.make_async_copy(src, dst, sems.at[i])
        for i, (src, dst) in enumerate(
            ((feat_hbm, feat), (lw_hbm, lw), (gum_hbm, gum), (cb_hbm, cb), (wt_hbm, wt))
        )
    ]
    for copy in copies:
        copy.start()
    copies[0].wait()
    copies[1].wait()
    logits = jnp.dot(feat[...], lw[...], preferred_element_type=F32)
    first = lax.broadcasted_iota(I32, (logits.shape[0], 128), 1) < V % 128
    copies[2].wait()
    soft = group_softmax((logits + gum[...]) / GUMBEL_SOFTNESS, first)
    middle = soft[:, 256:384]
    soft_low = jnp.concatenate([soft[:, :256], jnp.where(first, middle, 0.0)], axis=1)
    soft_high = jnp.concatenate([jnp.where(first, 0.0, middle), soft[:, 384:]], axis=1)
    copies[3].wait()
    codevec = jnp.concatenate(
        [
            jnp.dot(part.astype(BF16), cb[at : at + 384, :], preferred_element_type=F32)
            for part, at in ((soft_low, 0), (soft_high, 256))
        ],
        axis=1,
    ).astype(BF16)
    copies[4].wait()
    target = lax.dot_general(
        wt[...], codevec, (((1,), (1,)), ((), ())), preferred_element_type=F32
    )
    width = target.shape[0]
    tgt_ref[0:width, :] = target.astype(BF16)
    probs = jnp.sum(group_softmax(logits, first), axis=0, keepdims=True)
    tgt_ref[width:, :] = jnp.concatenate(
        [
            part[:, at : at + 128]
            for part in bf16_parts(probs)
            for at in range(0, G * V, 128)
        ]
        + [jnp.zeros((1, 128), F32)],
        axis=0,
    ).astype(BF16)


def prepare_kernel(
    ctxt_hbm, mask_hbm, idxt_hbm, tgt_ref, rows_ref, ctx_ref, code_kt_ref, code_tk_ref,
    ctxt, mask, idxt, sems,
):
    copies = [
        pltpu.make_async_copy(src, dst, sems.at[i])
        for i, (src, dst) in enumerate(
            ((ctxt_hbm, ctxt), (mask_hbm, mask), (idxt_hbm, idxt.at[pl.ds(0, NEG)]))
        )
    ]
    for copy in copies:
        copy.start()
    own = lax.axis_index("frames")
    partner = 1 - 2 * lax.rem(own, 2)
    inner = 2 - 4 * lax.rem(own // 2, 2)
    distances = (partner, inner, -inner, -3 * partner, inner + partner, partner - inner)
    for copy in copies:
        copy.wait()
    wide = tgt_ref[0 : ctxt.shape[0], :].astype(F32)
    context = ctxt[...].astype(F32)
    rows_ref[...] = jnp.zeros_like(rows_ref)
    rows_ref[0:1, :] = jnp.sum(wide * context, axis=0, keepdims=True)
    rows_ref[1:2, :] = jnp.sum(context * context, axis=0, keepdims=True)
    rows_ref[2:3, :] = jnp.sum(wide * wide, axis=0, keepdims=True)
    rows_ref[3:4, :] = mask[...].astype(F32)
    ctx_ref[...] = jnp.transpose(context).astype(BF16)
    row = lax.broadcasted_iota(I32, idxt.shape, 0)
    index = jnp.where(row < NEG, idxt[...], 0)
    offset = (((index >> 7) - own + 32) & 63) - 32
    block = jnp.zeros_like(index)
    for i, o in enumerate(distances):
        block = jnp.where(offset == o, i, block)
    code = (index & 127) + (block << 7)
    code_kt_ref[...] = code
    code_tk_ref[...] = jnp.transpose(code)


def lane_pick(values, index):
    return jnp.take_along_axis(values, index, axis=1, mode="promise_in_bounds")


def pick(picked, block, local, sims, which):
    return jnp.where(block == which, lane_pick(sims, local), picked)


def first_dots_kernel(
    own_ref, a_ref, b_ref, c_ref, ctx_ref, code_ref, picked_ref, norms_ref, probs_ref
):
    ctx = ctx_ref[...]
    width = ctx.shape[1]
    code = code_ref[...]
    local = code & 127
    block = code >> 7
    picked = jnp.zeros(code.shape, F32)
    probs = own_ref[width:, :].astype(F32)
    norms_ref[...] = jnp.zeros_like(norms_ref)
    for i, ref in ((1, a_ref), (2, b_ref), (3, c_ref)):
        target = ref[0:width, :]
        sims = jnp.dot(ctx, target, preferred_element_type=F32)
        picked = pick(picked, block, local, sims, i)
        wide = target.astype(F32)
        norms_ref[i : i + 1, :] = jnp.sum(wide * wide, axis=0, keepdims=True)
        probs = probs + ref[width:, :].astype(F32)
    picked_ref[...] = picked
    probs_ref[...] = probs


def dots_kernel(
    picked_ref, norms_ref, own_probs_ref, swap_ref, ctx_ref, code_ref, rows_ref,
    out_ref, probs_ref,
):
    ctx = ctx_ref[...]
    width = ctx.shape[1]
    code = code_ref[...]
    local = code & 127
    block = code >> 7
    out_ref[SELF_ROW : SELF_ROW + 4, :] = rows_ref[0:4, :]
    out_ref[NORM_ROW:, :] = norms_ref[...]
    tall = width + PROB_ROWS
    picked = picked_ref[...]
    probs = own_probs_ref[...] + swap_ref[3 * tall :, :].astype(F32)
    for i, at in ((4, 0), (5, tall), (0, 2 * tall)):
        target = swap_ref[at : at + width, :]
        sims = jnp.dot(ctx, target, preferred_element_type=F32)
        picked = pick(picked, block, local, sims, i)
        wide = target.astype(F32)
        out_ref[NORM_ROW + i : NORM_ROW + i + 1, :] = jnp.sum(wide * wide, axis=0, keepdims=True)
        probs = probs + swap_ref[at + width : at + tall, :].astype(F32)
    out_ref[0:NEG, :] = jnp.transpose(picked)[0:NEG, :]
    probs_ref[...] = jnp.zeros_like(probs_ref)
    probs_ref[0:5, :] = probs[0:5, :] + (probs[5:10, :] + probs[10:15, :])


def scores_kernel(p0, p1, p2, p3, code_ref, rows_ref, probs_ref, scores_ref, parts_ref):
    total = (p0[...] + p1[...]) + (p2[...] + p3[...])
    scale = lax.rsqrt(total[CTX_ROW : CTX_ROW + 1, :] + NORM_EPSILON) / LOGIT_SOFTNESS
    inverse = lax.rsqrt(total[OWN_NORM_ROW:, :] + NORM_EPSILON)
    own = total[SELF_ROW : SELF_ROW + 1, :] * inverse[0:1, :] * scale
    code = code_ref[0:104, :]
    local = code & 127
    block = code >> 7
    picked = jnp.zeros(code.shape, F32)
    for i in range(BLOCKS):
        at = NORM_ROW - OWN_NORM_ROW + i
        table = jnp.broadcast_to(inverse[at : at + 1, :], code.shape)
        picked = jnp.where(block == i, lane_pick(table, local), picked)
    others = total[0:104, :] * picked * scale
    row = lax.broadcasted_iota(I32, others.shape, 0)
    powers = jnp.where(row < NEG, jnp.exp(jnp.where(row < NEG, others, 0.0)), 0.0)
    summed = jnp.sum(powers, axis=0, keepdims=True) + jnp.exp(own)
    cross = jnp.where(rows_ref[3:4, :] == 1.0, jnp.log(summed) - own, 0.0)
    scores_ref[0:1, :] = own
    scores_ref[1 : NEG + 1, :] = others[0:NEG, :]
    cut = lax.rem(lax.axis_index("frames"), CLASSES)
    rolled = pltpu.roll(probs_ref[...], 128 - CUT * cut, 1)
    row = lax.broadcasted_iota(I32, rolled.shape, 0)
    lane = lax.broadcasted_iota(I32, rolled.shape, 1)
    line = jnp.where((lane >> 4) + row == 0, rolled, 0.0)
    for i in range(1, G * V // 128):
        here = ((lane >> 4) == i) & (row == i)
        line = jnp.where(here, pltpu.roll(rolled, CUT * i, 1), line)
    line = jnp.sum(line, axis=0, keepdims=True)
    lane = lax.broadcasted_iota(I32, line.shape, 1)
    line = jnp.where(
        lane < LOSS_LANE, line,
        jnp.where(lane == LOSS_LANE, jnp.sum(cross, axis=1, keepdims=True), 0.0),
    )
    parts_ref[...] = jnp.broadcast_to(line[None], parts_ref.shape)


def totals_kernel(frames, parts_ref, held_ref, scores_ref, loss_ref, diversity_ref):
    scores_ref[...] = held_ref[...]
    parts = parts_ref[...]
    parts = parts.reshape(parts.shape[0] // CLASSES, CLASSES, 1, 128)
    total = jnp.sum(parts, axis=0) / frames
    cut = lax.broadcasted_iota(I32, total.shape, 0)
    lane = lax.broadcasted_iota(I32, total.shape, 2)
    column = (lane >> 4) * 128 + cut * CUT + (lane & 15)
    counted = lane < LOSS_LANE
    usage = jnp.where(counted, total, 0.0)
    terms = usage * jnp.log(usage + 1e-07)

    def summed(where):
        rows = jnp.sum(jnp.where(where, terms, 0.0), axis=0)
        return jnp.sum(rows, axis=1, keepdims=True)

    perplex = jnp.exp(-summed(column < V)) + jnp.exp(-summed(column >= V))
    diversity_ref[...] = (G * V - perplex) / (G * V)
    loss = jnp.sum(jnp.where(lane == LOSS_LANE, total, 0.0), axis=0)
    loss_ref[...] = jnp.sum(loss, axis=1, keepdims=True)


def struct(shape, kind):
    return jax.ShapeDtypeStruct(shape, kind)


def exchange(value, shards, replicas, source):
    pairs = []
    for s in range(shards):
        for j in range(replicas):
            pairs.append((source(s) % shards * replicas + j, s * replicas + j))
    return lax.ppermute(value, ("frames", "mp"), pairs)


def on_device(
    features, logit_weight, gumbel, codebook, project_weight, context, distractors, masked
):
    count = features.shape[0]
    shards = lax.axis_size("frames")
    replicas = lax.axis_size("mp")
    weight_t = project_weight.T
    context_t = context.T
    width = context_t.shape[0]
    operands = (features, logit_weight, gumbel, codebook, weight_t)
    target = pl.pallas_call(
        target_kernel,
        out_shape=struct((width + PROB_ROWS, count), BF16),
        in_specs=[pl.BlockSpec(memory_space=HBM)] * 5,
        out_specs=pl.BlockSpec(memory_space=VMEM),
        scratch_shapes=[pltpu.VMEM(x.shape, x.dtype) for x in operands]
        + [pltpu.SemaphoreType.DMA((5,))],
        compiler_params=PARAMS,
        name="target",
    )(*[pltpu.with_memory_space_constraint(x, HBM) for x in operands])
    operands = (context_t, masked.reshape(1, count))
    rows, ctx, code_kt, code_tk = pl.pallas_call(
        prepare_kernel,
        out_shape=(
            struct((8, count), F32),
            struct((count, width), BF16),
            struct((128, count), I32),
            struct((count, 128), I32),
        ),
        in_specs=[pl.BlockSpec(memory_space=HBM)] * 3 + [pl.BlockSpec(memory_space=VMEM)],
        out_specs=[pl.BlockSpec(memory_space=VMEM)] * 4,
        scratch_shapes=[pltpu.VMEM(x.shape, x.dtype) for x in operands]
        + [pltpu.VMEM((128, count), I32), pltpu.SemaphoreType.DMA((3,))],
        compiler_params=PARAMS,
        name="prepare",
    )(*[pltpu.with_memory_space_constraint(x, HBM) for x in (*operands, distractors.T)], target)

    def outer(s):
        return s - 2 if s // 2 % 2 == 0 else s + 2

    def across(s):
        return s - 3 if s % 2 == 0 else s + 3

    send = functools.partial(exchange, shards=shards, replicas=replicas)
    b = send(target, source=outer)
    c = send(target, source=across)
    a = send(target, source=lambda s: s ^ 2)
    a, b, c = lax.optimization_barrier((a, b, c))
    swap = send(jnp.concatenate([a, b, target, c[width:]], axis=0), source=lambda s: s ^ 1)
    picked, norms, probs = pl.pallas_call(
        first_dots_kernel,
        out_shape=(
            struct((count, 128), F32),
            struct((PAYLOAD_ROWS - NORM_ROW, count), F32),
            struct((PROB_ROWS, 128), F32),
        ),
        in_specs=[pl.BlockSpec(memory_space=VMEM)] * 6,
        out_specs=[pl.BlockSpec(memory_space=VMEM)] * 3,
        compiler_params=PARAMS,
        name="first_dots",
    )(target, a, b, c, ctx, code_tk)
    payload, probs = pl.pallas_call(
        dots_kernel,
        out_shape=(struct((PAYLOAD_ROWS, count), F32), struct((8, 128), F32)),
        in_specs=[pl.BlockSpec(memory_space=VMEM)] * 7,
        out_specs=[pl.BlockSpec(memory_space=VMEM)] * 2,
        compiler_params=PARAMS,
        name="dots",
    )(picked, norms, probs, swap, ctx, code_tk, rows)
    peers = []
    for step in (2, 3, 1):
        peers.append(lax.ppermute(payload, "mp", [(j ^ step, j) for j in range(replicas)]))
    scores_t, parts = pl.pallas_call(
        scores_kernel,
        out_shape=(struct((NEG + 1, count), F32), struct((shards, 1, 128), F32)),
        in_specs=[pl.BlockSpec(memory_space=VMEM)] * 7,
        out_specs=[pl.BlockSpec(memory_space=VMEM)] * 2,
        compiler_params=PARAMS,
        name="scores",
    )(payload, *peers, code_kt, rows, probs)
    parts = lax.all_to_all(parts, "frames", split_axis=0, concat_axis=0, tiled=True)
    scores_t, loss, diversity = pl.pallas_call(
        functools.partial(totals_kernel, count * shards),
        out_shape=(struct(scores_t.shape, F32), struct((1, 1), F32), struct((1, 1), F32)),
        in_specs=[pl.BlockSpec(memory_space=VMEM)] * 2,
        out_specs=[pl.BlockSpec(memory_space=VMEM)] * 3,
        compiler_params=PARAMS,
        name="totals",
    )(parts, scores_t)
    return scores_t.T, loss.reshape(()), diversity.reshape(())


def solution(mesh):
    return jax.shard_map(
        on_device,
        mesh=mesh,
        in_specs=(
            P("frames", None),
            P(),
            P("frames", None),
            P(),
            P(None, "mp"),
            P("frames", "mp"),
            P("frames", None),
            P("frames"),
        ),
        out_specs=(P("frames", None), P(), P()),
        check_vma=False,
    )
```

```python
import functools

import jax
import jax.numpy as jnp
from jax import lax
from jax.experimental import pallas as pl
from jax.experimental.pallas import tpu as pltpu
from jax.sharding import PartitionSpec as P


V = 320
G = 2
NEG = 100
GUMBEL_SOFTNESS = 2.0
LOGIT_SOFTNESS = 0.1
NORM_EPSILON = 1e-06

F32 = jnp.float32
BF16 = jnp.bfloat16
I32 = jnp.int32

BLOCKS = 6

SELF_ROW = 100
CTX_ROW = 101
OWN_NORM_ROW = 102
NORM_ROW = 104
PAYLOAD_ROWS = 112

PROB_ROWS = 16
CLASSES = 8
CUT = 16
LOSS_LANE = 80

VMEM = pltpu.MemorySpace.VMEM
HBM = pltpu.MemorySpace.HBM
PARAMS = pltpu.CompilerParams(vmem_limit_bytes=8 << 20)


def group_stats(values, first, reduce, empty):
    head = values[:, : V - V % 128]
    middle = values[:, V - V % 128 : V - V % 128 + 128]
    tail = values[:, V - V % 128 + 128 :]
    low = reduce(
        jnp.concatenate([head, jnp.where(first, middle, empty)], axis=1), axis=1, keepdims=True
    )
    high = reduce(
        jnp.concatenate([jnp.where(first, empty, middle), tail], axis=1), axis=1, keepdims=True
    )
    return low, high


def by_group(low, high, first):
    count = first.shape[0]
    return jnp.concatenate(
        [
            jnp.broadcast_to(low, (count, V - V % 128)),
            jnp.where(first, low, high),
            jnp.broadcast_to(high, (count, V - V % 128)),
        ],
        axis=1,
    )


def group_softmax(values, first):
    shift = by_group(*group_stats(values, first, jnp.max, -jnp.inf), first)
    powers = jnp.exp(values - shift)
    low, high = group_stats(powers, first, jnp.sum, 0.0)
    return powers * by_group(1.0 / low, 1.0 / high, first)


def bf16_parts(values):
    high = values.astype(BF16).astype(F32)
    middle = (values - high).astype(BF16).astype(F32)
    return high, middle, values - high - middle


def target_kernel(feat_hbm, lw_hbm, gum_hbm, cb_hbm, wt_hbm, tgt_ref, feat, lw, gum, cb, wt, sems):
    copies = [
        pltpu.make_async_copy(src, dst, sems.at[i])
        for i, (src, dst) in enumerate(
            ((feat_hbm, feat), (lw_hbm, lw), (gum_hbm, gum), (cb_hbm, cb), (wt_hbm, wt))
        )
    ]
    for copy in copies:
        copy.start()
    copies[0].wait()
    copies[1].wait()
    logits = jnp.dot(feat[...], lw[...], preferred_element_type=F32)
    first = lax.broadcasted_iota(I32, (logits.shape[0], 128), 1) < V % 128
    copies[2].wait()
    soft = group_softmax((logits + gum[...]) / GUMBEL_SOFTNESS, first)
    middle = soft[:, 256:384]
    soft_low = jnp.concatenate([soft[:, :256], jnp.where(first, middle, 0.0)], axis=1)
    soft_high = jnp.concatenate([jnp.where(first, 0.0, middle), soft[:, 384:]], axis=1)
    copies[3].wait()
    codevec = jnp.concatenate(
        [
            jnp.dot(part.astype(BF16), cb[at : at + 384, :], preferred_element_type=F32)
            for part, at in ((soft_low, 0), (soft_high, 256))
        ],
        axis=1,
    ).astype(BF16)
    copies[4].wait()
    target = lax.dot_general(
        wt[...], codevec, (((1,), (1,)), ((), ())), preferred_element_type=F32
    )
    width = target.shape[0]
    tgt_ref[0:width, :] = target.astype(BF16)
    probs = jnp.sum(group_softmax(logits, first), axis=0, keepdims=True)
    tgt_ref[width:, :] = jnp.concatenate(
        [
            part[:, at : at + 128]
            for part in bf16_parts(probs)
            for at in range(0, G * V, 128)
        ]
        + [jnp.zeros((1, 128), F32)],
        axis=0,
    ).astype(BF16)


def prepare_kernel(
    ctxt_hbm, mask_hbm, idxt_hbm, tgt_ref, rows_ref, ctx_ref, code_kt_ref, code_tk_ref,
    ctxt, mask, idxt, sems,
):
    copies = [
        pltpu.make_async_copy(src, dst, sems.at[i])
        for i, (src, dst) in enumerate(
            ((ctxt_hbm, ctxt), (mask_hbm, mask), (idxt_hbm, idxt.at[pl.ds(0, NEG)]))
        )
    ]
    for copy in copies:
        copy.start()
    own = lax.axis_index("frames")
    partner = 1 - 2 * lax.rem(own, 2)
    inner = 2 - 4 * lax.rem(own // 2, 2)
    distances = (partner, inner, -inner, -3 * partner, inner + partner, partner - inner)
    for copy in copies:
        copy.wait()
    wide = tgt_ref[0 : ctxt.shape[0], :].astype(F32)
    context = ctxt[...].astype(F32)
    rows_ref[...] = jnp.zeros_like(rows_ref)
    rows_ref[0:1, :] = jnp.sum(wide * context, axis=0, keepdims=True)
    rows_ref[1:2, :] = jnp.sum(context * context, axis=0, keepdims=True)
    rows_ref[2:3, :] = jnp.sum(wide * wide, axis=0, keepdims=True)
    rows_ref[3:4, :] = mask[...].astype(F32)
    ctx_ref[...] = jnp.transpose(context).astype(BF16)
    row = lax.broadcasted_iota(I32, idxt.shape, 0)
    index = jnp.where(row < NEG, idxt[...], 0)
    offset = (((index >> 7) - own + 32) & 63) - 32
    block = jnp.zeros_like(index)
    for i, o in enumerate(distances):
        block = jnp.where(offset == o, i, block)
    code = (index & 127) + (block << 7)
    code_kt_ref[...] = code
    code_tk_ref[...] = jnp.transpose(code)


def lane_pick(values, index):
    return jnp.take_along_axis(values, index, axis=1, mode="promise_in_bounds")


def pick(picked, block, local, sims, which):
    return jnp.where(block == which, lane_pick(sims, local), picked)


def first_dots_kernel(own_ref, a_ref, b_ref, ctx_ref, code_ref, picked_ref, norms_ref, probs_ref):
    ctx = ctx_ref[...]
    width = ctx.shape[1]
    code = code_ref[...]
    local = code & 127
    block = code >> 7
    picked = jnp.zeros(code.shape, F32)
    probs = own_ref[width:, :].astype(F32)
    norms_ref[...] = jnp.zeros_like(norms_ref)
    for i, ref in ((1, a_ref), (2, b_ref)):
        target = ref[0:width, :]
        sims = jnp.dot(ctx, target, preferred_element_type=F32)
        picked = pick(picked, block, local, sims, i)
        wide = target.astype(F32)
        norms_ref[i : i + 1, :] = jnp.sum(wide * wide, axis=0, keepdims=True)
        probs = probs + ref[width:, :].astype(F32)
    picked_ref[...] = picked
    probs_ref[...] = probs


def dots_kernel(
    picked_ref, norms_ref, own_probs_ref, swap_ref, c_ref, ctx_ref, code_ref, rows_ref,
    out_ref, probs_ref, edge_ref,
):
    ctx = ctx_ref[...]
    width = ctx.shape[1]
    code = code_ref[...]
    local = code & 127
    block = code >> 7
    out_ref[SELF_ROW : SELF_ROW + 4, :] = rows_ref[0:4, :]
    out_ref[NORM_ROW:, :] = norms_ref[...]
    tall = width + PROB_ROWS
    picked = picked_ref[...]
    edge = c_ref[width:, :].astype(F32)
    edge_ref[...] = edge
    probs = own_probs_ref[...] + edge
    for i, ref, at in ((4, swap_ref, 0), (5, swap_ref, tall), (0, swap_ref, 2 * tall), (3, c_ref, 0)):
        target = ref[at : at + width, :]
        sims = jnp.dot(ctx, target, preferred_element_type=F32)
        picked = pick(picked, block, local, sims, i)
        wide = target.astype(F32)
        out_ref[NORM_ROW + i : NORM_ROW + i + 1, :] = jnp.sum(wide * wide, axis=0, keepdims=True)
        if i != 3:
            probs = probs + ref[at + width : at + tall, :].astype(F32)
    out_ref[0:NEG, :] = jnp.transpose(picked)[0:NEG, :]
    probs_ref[...] = probs


def scores_kernel(p0, p1, p2, p3, code_ref, rows_ref, probs_ref, edge_ref, scores_ref, parts_ref):
    total = (p0[...] + p1[...]) + (p2[...] + p3[...])
    scale = lax.rsqrt(total[CTX_ROW : CTX_ROW + 1, :] + NORM_EPSILON) / LOGIT_SOFTNESS
    inverse = lax.rsqrt(total[OWN_NORM_ROW:, :] + NORM_EPSILON)
    own = total[SELF_ROW : SELF_ROW + 1, :] * inverse[0:1, :] * scale
    code = code_ref[0:104, :]
    local = code & 127
    block = code >> 7
    picked = jnp.zeros(code.shape, F32)
    for i in range(BLOCKS):
        at = NORM_ROW - OWN_NORM_ROW + i
        table = jnp.broadcast_to(inverse[at : at + 1, :], code.shape)
        picked = jnp.where(block == i, lane_pick(table, local), picked)
    others = total[0:104, :] * picked * scale
    row = lax.broadcasted_iota(I32, others.shape, 0)
    powers = jnp.where(row < NEG, jnp.exp(jnp.where(row < NEG, others, 0.0)), 0.0)
    summed = jnp.sum(powers, axis=0, keepdims=True) + jnp.exp(own)
    cross = jnp.where(rows_ref[3:4, :] == 1.0, jnp.log(summed) - own, 0.0)
    scores_ref[0:1, :] = own
    scores_ref[1 : NEG + 1, :] = others[0:NEG, :]
    cut = lax.rem(lax.axis_index("frames"), CLASSES)
    sums = probs_ref[...] + edge_ref[...]
    sums = jnp.concatenate(
        [sums[0:5, :] + (sums[5:10, :] + sums[10:15, :]), jnp.zeros((3, 128), F32)], axis=0
    )
    rolled = pltpu.roll(sums, 128 - CUT * cut, 1)
    row = lax.broadcasted_iota(I32, rolled.shape, 0)
    lane = lax.broadcasted_iota(I32, rolled.shape, 1)
    line = jnp.where((lane >> 4) + row == 0, rolled, 0.0)
    for i in range(1, G * V // 128):
        here = ((lane >> 4) == i) & (row == i)
        line = jnp.where(here, pltpu.roll(rolled, CUT * i, 1), line)
    line = jnp.sum(line, axis=0, keepdims=True)
    lane = lax.broadcasted_iota(I32, line.shape, 1)
    line = jnp.where(
        lane < LOSS_LANE, line,
        jnp.where(lane == LOSS_LANE, jnp.sum(cross, axis=1, keepdims=True), 0.0),
    )
    parts_ref[...] = jnp.broadcast_to(line[None], parts_ref.shape)


def totals_kernel(frames, parts_ref, held_ref, scores_ref, loss_ref, diversity_ref):
    scores_ref[...] = held_ref[...]
    parts = parts_ref[...]
    parts = parts.reshape(parts.shape[0] // CLASSES, CLASSES, 1, 128)
    total = jnp.sum(parts, axis=0) / frames
    cut = lax.broadcasted_iota(I32, total.shape, 0)
    lane = lax.broadcasted_iota(I32, total.shape, 2)
    column = (lane >> 4) * 128 + cut * CUT + (lane & 15)
    counted = lane < LOSS_LANE
    usage = jnp.where(counted, total, 0.0)
    terms = usage * jnp.log(usage + 1e-07)

    def summed(where):
        rows = jnp.sum(jnp.where(where, terms, 0.0), axis=0)
        return jnp.sum(rows, axis=1, keepdims=True)

    perplex = jnp.exp(-summed(column < V)) + jnp.exp(-summed(column >= V))
    diversity_ref[...] = (G * V - perplex) / (G * V)
    loss = jnp.sum(jnp.where(lane == LOSS_LANE, total, 0.0), axis=0)
    loss_ref[...] = jnp.sum(loss, axis=1, keepdims=True)


def struct(shape, kind):
    return jax.ShapeDtypeStruct(shape, kind)


def exchange(value, shards, replicas, source):
    pairs = []
    for s in range(shards):
        for j in range(replicas):
            pairs.append((source(s) % shards * replicas + j, s * replicas + j))
    return lax.ppermute(value, ("frames", "mp"), pairs)


def on_device(
    features, logit_weight, gumbel, codebook, project_weight, context, distractors, masked
):
    count = features.shape[0]
    shards = lax.axis_size("frames")
    replicas = lax.axis_size("mp")
    weight_t = project_weight.T
    context_t = context.T
    width = context_t.shape[0]
    operands = (features, logit_weight, gumbel, codebook, weight_t)
    target = pl.pallas_call(
        target_kernel,
        out_shape=struct((width + PROB_ROWS, count), BF16),
        in_specs=[pl.BlockSpec(memory_space=HBM)] * 5,
        out_specs=pl.BlockSpec(memory_space=VMEM),
        scratch_shapes=[pltpu.VMEM(x.shape, x.dtype) for x in operands]
        + [pltpu.SemaphoreType.DMA((5,))],
        compiler_params=PARAMS,
        name="target",
    )(*[pltpu.with_memory_space_constraint(x, HBM) for x in operands])
    operands = (context_t, masked.reshape(1, count))
    rows, ctx, code_kt, code_tk = pl.pallas_call(
        prepare_kernel,
        out_shape=(
            struct((8, count), F32),
            struct((count, width), BF16),
            struct((128, count), I32),
            struct((count, 128), I32),
        ),
        in_specs=[pl.BlockSpec(memory_space=HBM)] * 3 + [pl.BlockSpec(memory_space=VMEM)],
        out_specs=[pl.BlockSpec(memory_space=VMEM)] * 4,
        scratch_shapes=[pltpu.VMEM(x.shape, x.dtype) for x in operands]
        + [pltpu.VMEM((128, count), I32), pltpu.SemaphoreType.DMA((3,))],
        compiler_params=PARAMS,
        name="prepare",
    )(*[pltpu.with_memory_space_constraint(x, HBM) for x in (*operands, distractors.T)], target)

    def outer(s):
        return s - 2 if s // 2 % 2 == 0 else s + 2

    def across(s):
        return s - 3 if s % 2 == 0 else s + 3

    send = functools.partial(exchange, shards=shards, replicas=replicas)
    b = send(target, source=outer)
    c = send(target, source=across)
    a = send(target, source=lambda s: s ^ 2)
    swap = send(jnp.concatenate([a, b, target], axis=0), source=lambda s: s ^ 1)
    picked, norms, probs = pl.pallas_call(
        first_dots_kernel,
        out_shape=(
            struct((count, 128), F32),
            struct((PAYLOAD_ROWS - NORM_ROW, count), F32),
            struct((PROB_ROWS, 128), F32),
        ),
        in_specs=[pl.BlockSpec(memory_space=VMEM)] * 5,
        out_specs=[pl.BlockSpec(memory_space=VMEM)] * 3,
        compiler_params=PARAMS,
        name="first_dots",
    )(target, a, b, ctx, code_tk)
    payload, probs, edge = pl.pallas_call(
        dots_kernel,
        out_shape=(
            struct((PAYLOAD_ROWS, count), F32),
            struct((PROB_ROWS, 128), F32),
            struct((PROB_ROWS, 128), F32),
        ),
        in_specs=[pl.BlockSpec(memory_space=VMEM)] * 8,
        out_specs=[pl.BlockSpec(memory_space=VMEM)] * 3,
        compiler_params=PARAMS,
        name="dots",
    )(picked, norms, probs, swap, c, ctx, code_tk, rows)
    edge = send(edge, source=lambda s: s ^ 1)
    peers = []
    for step in (2, 3, 1):
        peers.append(lax.ppermute(payload, "mp", [(j ^ step, j) for j in range(replicas)]))
    scores_t, parts = pl.pallas_call(
        scores_kernel,
        out_shape=(struct((NEG + 1, count), F32), struct((shards, 1, 128), F32)),
        in_specs=[pl.BlockSpec(memory_space=VMEM)] * 8,
        out_specs=[pl.BlockSpec(memory_space=VMEM)] * 2,
        compiler_params=PARAMS,
        name="scores",
    )(payload, *peers, code_kt, rows, probs, edge)
    parts = lax.all_to_all(parts, "frames", split_axis=0, concat_axis=0, tiled=True)
    scores_t, loss, diversity = pl.pallas_call(
        functools.partial(totals_kernel, count * shards),
        out_shape=(struct(scores_t.shape, F32), struct((1, 1), F32), struct((1, 1), F32)),
        in_specs=[pl.BlockSpec(memory_space=VMEM)] * 2,
        out_specs=[pl.BlockSpec(memory_space=VMEM)] * 3,
        compiler_params=PARAMS,
        name="totals",
    )(parts, scores_t)
    return scores_t.T, loss.reshape(()), diversity.reshape(())


def solution(mesh):
    return jax.shard_map(
        on_device,
        mesh=mesh,
        in_specs=(
            P("frames", None),
            P(),
            P("frames", None),
            P(),
            P(None, "mp"),
            P("frames", "mp"),
            P("frames", None),
            P("frames"),
        ),
        out_specs=(P("frames", None), P(), P()),
        check_vma=False,
    )
```

```python
import functools

import jax
import jax.numpy as jnp
from jax import lax
from jax.experimental import pallas as pl
from jax.experimental.pallas import tpu as pltpu
from jax.sharding import PartitionSpec as P


V = 320
G = 2
NEG = 100
GUMBEL_SOFTNESS = 2.0
LOGIT_SOFTNESS = 0.1
NORM_EPSILON = 1e-06

F32 = jnp.float32
BF16 = jnp.bfloat16
I32 = jnp.int32

BLOCKS = 6

SELF_ROW = 100
CTX_ROW = 101
OWN_NORM_ROW = 102
NORM_ROW = 104
PAYLOAD_ROWS = 112

PROB_ROWS = 16
CLASSES = 8
CUT = 16
LOSS_LANE = 80

VMEM = pltpu.MemorySpace.VMEM
HBM = pltpu.MemorySpace.HBM
PARAMS = pltpu.CompilerParams(vmem_limit_bytes=8 << 20)


def group_stats(values, first, reduce, empty):
    head = values[:, : V - V % 128]
    middle = values[:, V - V % 128 : V - V % 128 + 128]
    tail = values[:, V - V % 128 + 128 :]
    low = reduce(
        jnp.concatenate([head, jnp.where(first, middle, empty)], axis=1), axis=1, keepdims=True
    )
    high = reduce(
        jnp.concatenate([jnp.where(first, empty, middle), tail], axis=1), axis=1, keepdims=True
    )
    return low, high


def by_group(low, high, first):
    count = first.shape[0]
    return jnp.concatenate(
        [
            jnp.broadcast_to(low, (count, V - V % 128)),
            jnp.where(first, low, high),
            jnp.broadcast_to(high, (count, V - V % 128)),
        ],
        axis=1,
    )


def group_softmax(values, first):
    shift = by_group(*group_stats(values, first, jnp.max, -jnp.inf), first)
    powers = jnp.exp(values - shift)
    low, high = group_stats(powers, first, jnp.sum, 0.0)
    return powers * by_group(1.0 / low, 1.0 / high, first)


def bf16_parts(values):
    high = values.astype(BF16).astype(F32)
    middle = (values - high).astype(BF16).astype(F32)
    return high, middle, values - high - middle


def target_kernel(feat_hbm, lw_hbm, gum_hbm, cb_hbm, wt_hbm, tgt_ref, feat, lw, gum, cb, wt, sems):
    copies = [
        pltpu.make_async_copy(src, dst, sems.at[i])
        for i, (src, dst) in enumerate(
            ((feat_hbm, feat), (lw_hbm, lw), (gum_hbm, gum), (cb_hbm, cb), (wt_hbm, wt))
        )
    ]
    for copy in copies:
        copy.start()
    copies[0].wait()
    copies[1].wait()
    logits = jnp.dot(feat[...], lw[...], preferred_element_type=F32)
    first = lax.broadcasted_iota(I32, (logits.shape[0], 128), 1) < V % 128
    copies[2].wait()
    soft = group_softmax((logits + gum[...]) / GUMBEL_SOFTNESS, first)
    middle = soft[:, 256:384]
    soft_low = jnp.concatenate([soft[:, :256], jnp.where(first, middle, 0.0)], axis=1)
    soft_high = jnp.concatenate([jnp.where(first, 0.0, middle), soft[:, 384:]], axis=1)
    copies[3].wait()
    codevec = jnp.concatenate(
        [
            jnp.dot(part.astype(BF16), cb[at : at + 384, :], preferred_element_type=F32)
            for part, at in ((soft_low, 0), (soft_high, 256))
        ],
        axis=1,
    ).astype(BF16)
    copies[4].wait()
    target = lax.dot_general(
        wt[...], codevec, (((1,), (1,)), ((), ())), preferred_element_type=F32
    )
    width = target.shape[0]
    tgt_ref[0:width, :] = target.astype(BF16)
    probs = jnp.sum(group_softmax(logits, first), axis=0, keepdims=True)
    tgt_ref[width:, :] = jnp.concatenate(
        [
            part[:, at : at + 128]
            for part in bf16_parts(probs)
            for at in range(0, G * V, 128)
        ]
        + [jnp.zeros((1, 128), F32)],
        axis=0,
    ).astype(BF16)


def prepare_kernel(
    ctxt_hbm, mask_hbm, idxt_hbm, tgt_ref, rows_ref, ctx_ref, code_kt_ref, code_tk_ref,
    ctxt, mask, idxt, sems,
):
    copies = [
        pltpu.make_async_copy(src, dst, sems.at[i])
        for i, (src, dst) in enumerate(
            ((ctxt_hbm, ctxt), (mask_hbm, mask), (idxt_hbm, idxt.at[pl.ds(0, NEG)]))
        )
    ]
    for copy in copies:
        copy.start()
    own = lax.axis_index("frames")
    partner = 1 - 2 * lax.rem(own, 2)
    inner = 2 - 4 * lax.rem(own // 2, 2)
    distances = (partner, inner, -inner, -3 * partner, inner + partner, partner - inner)
    for copy in copies:
        copy.wait()
    wide = tgt_ref[0 : ctxt.shape[0], :].astype(F32)
    context = ctxt[...].astype(F32)
    rows_ref[...] = jnp.zeros_like(rows_ref)
    rows_ref[0:1, :] = jnp.sum(wide * context, axis=0, keepdims=True)
    rows_ref[1:2, :] = jnp.sum(context * context, axis=0, keepdims=True)
    rows_ref[2:3, :] = jnp.sum(wide * wide, axis=0, keepdims=True)
    rows_ref[3:4, :] = mask[...].astype(F32)
    ctx_ref[...] = jnp.transpose(context).astype(BF16)
    row = lax.broadcasted_iota(I32, idxt.shape, 0)
    index = jnp.where(row < NEG, idxt[...], 0)
    offset = (((index >> 7) - own + 32) & 63) - 32
    block = jnp.zeros_like(index)
    for i, o in enumerate(distances):
        block = jnp.where(offset == o, i, block)
    code = (index & 127) + (block << 7)
    code_kt_ref[...] = code
    code_tk_ref[...] = jnp.transpose(code)


def lane_pick(values, index):
    return jnp.take_along_axis(values, index, axis=1, mode="promise_in_bounds")


def pick(picked, block, local, sims, which):
    return jnp.where(block == which, lane_pick(sims, local), picked)


def first_dots_kernel(own_ref, a_ref, b_ref, ctx_ref, code_ref, picked_ref, norms_ref, probs_ref):
    ctx = ctx_ref[...]
    width = ctx.shape[1]
    code = code_ref[...]
    local = code & 127
    block = code >> 7
    picked = jnp.zeros(code.shape, F32)
    probs = own_ref[width:, :].astype(F32)
    norms_ref[...] = jnp.zeros_like(norms_ref)
    for i, ref in ((1, a_ref), (2, b_ref)):
        target = ref[0:width, :]
        sims = jnp.dot(ctx, target, preferred_element_type=F32)
        picked = pick(picked, block, local, sims, i)
        wide = target.astype(F32)
        norms_ref[i : i + 1, :] = jnp.sum(wide * wide, axis=0, keepdims=True)
        probs = probs + ref[width:, :].astype(F32)
    picked_ref[...] = picked
    probs_ref[...] = probs


def dots_kernel(
    picked_ref, norms_ref, own_probs_ref, swap_ref, c_ref, ctx_ref, code_ref, rows_ref,
    out_ref, probs_ref, edge_ref,
):
    ctx = ctx_ref[...]
    width = ctx.shape[1]
    code = code_ref[...]
    local = code & 127
    block = code >> 7
    out_ref[SELF_ROW : SELF_ROW + 4, :] = rows_ref[0:4, :]
    out_ref[NORM_ROW:, :] = norms_ref[...]
    tall = width + PROB_ROWS
    picked = picked_ref[...]
    edge = c_ref[width:, :].astype(F32)
    edge_ref[...] = edge
    probs = own_probs_ref[...] + edge
    for i, ref, at in ((4, swap_ref, 0), (5, swap_ref, tall), (0, swap_ref, 2 * tall), (3, c_ref, 0)):
        target = ref[at : at + width, :]
        sims = jnp.dot(ctx, target, preferred_element_type=F32)
        picked = pick(picked, block, local, sims, i)
        wide = target.astype(F32)
        out_ref[NORM_ROW + i : NORM_ROW + i + 1, :] = jnp.sum(wide * wide, axis=0, keepdims=True)
        if i != 3:
            probs = probs + ref[at + width : at + tall, :].astype(F32)
    out_ref[0:NEG, :] = jnp.transpose(picked)[0:NEG, :]
    probs_ref[...] = probs


def scores_kernel(p0, p1, p2, p3, code_ref, rows_ref, probs_ref, edge_ref, scores_ref, parts_ref):
    total = (p0[...].astype(F32) + p1[...].astype(F32)) + (
        p2[...].astype(F32) + p3[...].astype(F32)
    )
    scale = lax.rsqrt(total[CTX_ROW : CTX_ROW + 1, :] + NORM_EPSILON) / LOGIT_SOFTNESS
    inverse = lax.rsqrt(total[OWN_NORM_ROW:, :] + NORM_EPSILON)
    own = total[SELF_ROW : SELF_ROW + 1, :] * inverse[0:1, :] * scale
    code = code_ref[0:104, :]
    local = code & 127
    block = code >> 7
    picked = jnp.zeros(code.shape, F32)
    for i in range(BLOCKS):
        at = NORM_ROW - OWN_NORM_ROW + i
        table = jnp.broadcast_to(inverse[at : at + 1, :], code.shape)
        picked = jnp.where(block == i, lane_pick(table, local), picked)
    others = total[0:104, :] * picked * scale
    row = lax.broadcasted_iota(I32, others.shape, 0)
    powers = jnp.where(row < NEG, jnp.exp(jnp.where(row < NEG, others, 0.0)), 0.0)
    summed = jnp.sum(powers, axis=0, keepdims=True) + jnp.exp(own)
    cross = jnp.where(rows_ref[3:4, :] == 1.0, jnp.log(summed) - own, 0.0)
    scores_ref[0:1, :] = own
    scores_ref[1 : NEG + 1, :] = others[0:NEG, :]
    cut = lax.rem(lax.axis_index("frames"), CLASSES)
    sums = probs_ref[...] + edge_ref[...]
    sums = jnp.concatenate(
        [sums[0:5, :] + (sums[5:10, :] + sums[10:15, :]), jnp.zeros((3, 128), F32)], axis=0
    )
    rolled = pltpu.roll(sums, 128 - CUT * cut, 1)
    row = lax.broadcasted_iota(I32, rolled.shape, 0)
    lane = lax.broadcasted_iota(I32, rolled.shape, 1)
    line = jnp.where((lane >> 4) + row == 0, rolled, 0.0)
    for i in range(1, G * V // 128):
        here = ((lane >> 4) == i) & (row == i)
        line = jnp.where(here, pltpu.roll(rolled, CUT * i, 1), line)
    line = jnp.sum(line, axis=0, keepdims=True)
    lane = lax.broadcasted_iota(I32, line.shape, 1)
    line = jnp.where(
        lane < LOSS_LANE, line,
        jnp.where(lane == LOSS_LANE, jnp.sum(cross, axis=1, keepdims=True), 0.0),
    )
    parts_ref[...] = jnp.broadcast_to(line[None], parts_ref.shape)


def totals_kernel(frames, parts_ref, held_ref, scores_ref, loss_ref, diversity_ref):
    scores_ref[...] = held_ref[...]
    parts = parts_ref[...]
    parts = parts.reshape(parts.shape[0] // CLASSES, CLASSES, 1, 128)
    total = jnp.sum(parts, axis=0) / frames
    cut = lax.broadcasted_iota(I32, total.shape, 0)
    lane = lax.broadcasted_iota(I32, total.shape, 2)
    column = (lane >> 4) * 128 + cut * CUT + (lane & 15)
    counted = lane < LOSS_LANE
    usage = jnp.where(counted, total, 0.0)
    terms = usage * jnp.log(usage + 1e-07)

    def summed(where):
        rows = jnp.sum(jnp.where(where, terms, 0.0), axis=0)
        return jnp.sum(rows, axis=1, keepdims=True)

    perplex = jnp.exp(-summed(column < V)) + jnp.exp(-summed(column >= V))
    diversity_ref[...] = (G * V - perplex) / (G * V)
    loss = jnp.sum(jnp.where(lane == LOSS_LANE, total, 0.0), axis=0)
    loss_ref[...] = jnp.sum(loss, axis=1, keepdims=True)


def struct(shape, kind):
    return jax.ShapeDtypeStruct(shape, kind)


def exchange(value, shards, replicas, source):
    pairs = []
    for s in range(shards):
        for j in range(replicas):
            pairs.append((source(s) % shards * replicas + j, s * replicas + j))
    return lax.ppermute(value, ("frames", "mp"), pairs)


def on_device(
    features, logit_weight, gumbel, codebook, project_weight, context, distractors, masked
):
    count = features.shape[0]
    shards = lax.axis_size("frames")
    replicas = lax.axis_size("mp")
    weight_t = project_weight.T
    context_t = context.T
    width = context_t.shape[0]
    operands = (features, logit_weight, gumbel, codebook, weight_t)
    target = pl.pallas_call(
        target_kernel,
        out_shape=struct((width + PROB_ROWS, count), BF16),
        in_specs=[pl.BlockSpec(memory_space=HBM)] * 5,
        out_specs=pl.BlockSpec(memory_space=VMEM),
        scratch_shapes=[pltpu.VMEM(x.shape, x.dtype) for x in operands]
        + [pltpu.SemaphoreType.DMA((5,))],
        compiler_params=PARAMS,
        name="target",
    )(*[pltpu.with_memory_space_constraint(x, HBM) for x in operands])
    operands = (context_t, masked.reshape(1, count))
    rows, ctx, code_kt, code_tk = pl.pallas_call(
        prepare_kernel,
        out_shape=(
            struct((8, count), F32),
            struct((count, width), BF16),
            struct((128, count), I32),
            struct((count, 128), I32),
        ),
        in_specs=[pl.BlockSpec(memory_space=HBM)] * 3 + [pl.BlockSpec(memory_space=VMEM)],
        out_specs=[pl.BlockSpec(memory_space=VMEM)] * 4,
        scratch_shapes=[pltpu.VMEM(x.shape, x.dtype) for x in operands]
        + [pltpu.VMEM((128, count), I32), pltpu.SemaphoreType.DMA((3,))],
        compiler_params=PARAMS,
        name="prepare",
    )(*[pltpu.with_memory_space_constraint(x, HBM) for x in (*operands, distractors.T)], target)

    def outer(s):
        return s - 2 if s // 2 % 2 == 0 else s + 2

    def across(s):
        return s - 3 if s % 2 == 0 else s + 3

    send = functools.partial(exchange, shards=shards, replicas=replicas)
    b = send(target, source=outer)
    c = send(target, source=across)
    a = send(target, source=lambda s: s ^ 2)
    swap = send(jnp.concatenate([a, b, target], axis=0), source=lambda s: s ^ 1)
    picked, norms, probs = pl.pallas_call(
        first_dots_kernel,
        out_shape=(
            struct((count, 128), F32),
            struct((PAYLOAD_ROWS - NORM_ROW, count), F32),
            struct((PROB_ROWS, 128), F32),
        ),
        in_specs=[pl.BlockSpec(memory_space=VMEM)] * 5,
        out_specs=[pl.BlockSpec(memory_space=VMEM)] * 3,
        compiler_params=PARAMS,
        name="first_dots",
    )(target, a, b, ctx, code_tk)
    payload, probs, edge = pl.pallas_call(
        dots_kernel,
        out_shape=(
            struct((PAYLOAD_ROWS, count), F32),
            struct((PROB_ROWS, 128), F32),
            struct((PROB_ROWS, 128), F32),
        ),
        in_specs=[pl.BlockSpec(memory_space=VMEM)] * 8,
        out_specs=[pl.BlockSpec(memory_space=VMEM)] * 3,
        compiler_params=PARAMS,
        name="dots",
    )(picked, norms, probs, swap, c, ctx, code_tk, rows)
    edge = send(edge, source=lambda s: s ^ 1)
    narrow = payload.astype(BF16)
    peers = []
    for step in (2, 3, 1):
        peers.append(lax.ppermute(narrow, "mp", [(j ^ step, j) for j in range(replicas)]))
    scores_t, parts = pl.pallas_call(
        scores_kernel,
        out_shape=(struct((NEG + 1, count), F32), struct((shards, 1, 128), F32)),
        in_specs=[pl.BlockSpec(memory_space=VMEM)] * 8,
        out_specs=[pl.BlockSpec(memory_space=VMEM)] * 2,
        compiler_params=PARAMS,
        name="scores",
    )(narrow, *peers, code_kt, rows, probs, edge)
    parts = lax.all_to_all(parts, "frames", split_axis=0, concat_axis=0, tiled=True)
    scores_t, loss, diversity = pl.pallas_call(
        functools.partial(totals_kernel, count * shards),
        out_shape=(struct(scores_t.shape, F32), struct((1, 1), F32), struct((1, 1), F32)),
        in_specs=[pl.BlockSpec(memory_space=VMEM)] * 2,
        out_specs=[pl.BlockSpec(memory_space=VMEM)] * 3,
        compiler_params=PARAMS,
        name="totals",
    )(parts, scores_t)
    return scores_t.T, loss.reshape(()), diversity.reshape(())


def solution(mesh):
    return jax.shard_map(
        on_device,
        mesh=mesh,
        in_specs=(
            P("frames", None),
            P(),
            P("frames", None),
            P(),
            P(None, "mp"),
            P("frames", "mp"),
            P("frames", None),
            P("frames"),
        ),
        out_specs=(P("frames", None), P(), P()),
        check_vma=False,
    )
```
